128 devices in a mesh: dp: 1, tp: 2 (over core), sp: 64 (over z, y, x).
Axes of the slice: x: 4, y: 4, z: 4, core: 2. Of those that a mesh axis runs over, the one named last changes fastest.
Arguments:
- hidden: bfloat16 [2, 8192, 2048], P('dp', 'sp')
- bucket: int32 [2, 32, 8192], P('dp', 'tp', 'sp')
- w_qk: bfloat16 [2048, 32, 64], P(None, 'tp')
- w_v: bfloat16 [2048, 32, 64], P(None, 'tp')
- w_o: bfloat16 [32, 64, 2048], P('tp')
Outputs:
- output: bfloat16 [2, 8192, 2048], P('dp', 'sp', 'tp')
All inputs are finite; a program needn't handle non-finite values.
Results may differ from the reference program's by a relative error of at most 0.0144573.
Values are sent between devices in bfloat16 or wider.
A program may use at most 1 GiB of HBM per device.

```python
import jax
import jax.numpy as jnp
from jax import lax

BATCH = 2
TOK_DEV = 128
GROUP = 64
D_MODEL = 2048
HEADS = 32
HEAD_DIM = 64
CHUNK = 128

SEQ_LEN = TOK_DEV * GROUP
PER_RANGE = TOK_DEV // CHUNK
N_CHUNKS = SEQ_LEN // CHUNK
MASK_VALUE = -1e5


def draw_buckets(key):
    key_pair, key_shuffle, key_perm, key_fine = jax.random.split(key, 4)
    head_rows = BATCH * HEADS
    even_share = TOK_DEV // GROUP
    spread = jax.random.randint(key_pair, (head_rows, GROUP // 2), 0, even_share + 1)
    spread = spread.at[:, 0].set(even_share)
    shares = jnp.concatenate([even_share + spread, even_share - spread], axis=1)
    shares = jax.vmap(jax.random.permutation)(jax.random.split(key_shuffle, head_rows), shares)
    device_ids = jnp.arange(GROUP)
    pair_counts = shares[:, (device_ids[None, :] - device_ids[:, None]) % GROUP]
    bounds = jnp.cumsum(pair_counts, axis=2).reshape(head_rows * GROUP, GROUP)
    slot_ids = jnp.arange(TOK_DEV, dtype=jnp.int32)
    ranges = jax.vmap(lambda bound_row: jnp.searchsorted(bound_row, slot_ids, side="right"))(bounds)
    shuffles = jax.vmap(lambda perm_key: jax.random.permutation(perm_key, TOK_DEV))(jax.random.split(key_perm, head_rows * GROUP))
    ranges = jnp.take_along_axis(ranges, shuffles, axis=1)
    fine_ids = jax.random.randint(key_fine, (head_rows * GROUP, TOK_DEV), 0, PER_RANGE)
    return (ranges * PER_RANGE + fine_ids).astype(jnp.int32).reshape(BATCH, HEADS, SEQ_LEN)


def setup_inputs(seed: int = 0, part: int = 0) -> dict:
    key = jax.random.key(seed)
    key_hidden, key_bucket, key_qk, key_v, key_o = jax.random.split(key, 5)
    hidden = jax.random.normal(jax.random.fold_in(key_hidden, part), (BATCH, SEQ_LEN, D_MODEL), jnp.float32)
    bucket = draw_buckets(jax.random.fold_in(key_bucket, part))
    qk_scale = 2.0 * (HEAD_DIM / D_MODEL) ** 0.5
    in_scale = D_MODEL ** -0.5
    out_scale = (HEADS * HEAD_DIM) ** -0.5
    w_qk = jax.random.normal(key_qk, (D_MODEL, HEADS, HEAD_DIM), jnp.float32) * qk_scale
    w_v = jax.random.normal(key_v, (D_MODEL, HEADS, HEAD_DIM), jnp.float32) * in_scale
    w_o = jax.random.normal(key_o, (HEADS, HEAD_DIM, D_MODEL), jnp.float32) * out_scale
    return {"hidden": hidden.astype(jnp.bfloat16), "bucket": bucket, "w_qk": w_qk.astype(jnp.bfloat16), "w_v": w_v.astype(jnp.bfloat16), "w_o": w_o.astype(jnp.bfloat16)}


def head_attention(operands):
    qk_rows, v_rows, sort_keys = operands
    sort_order = jnp.argsort(sort_keys)
    sorted_rank = jnp.argsort(sort_order)
    q_wide = qk_rows[sort_order].astype(jnp.float32)
    key_unit = (q_wide / jnp.sqrt(jnp.sum(q_wide * q_wide, axis=-1, keepdims=True))).astype(jnp.bfloat16).astype(jnp.float32)
    v_wide = v_rows[sort_order].astype(jnp.float32)
    query_blk = q_wide.reshape(N_CHUNKS, CHUNK, HEAD_DIM)
    key_blk = key_unit.reshape(N_CHUNKS, CHUNK, HEAD_DIM)
    val_blk = v_wide.reshape(N_CHUNKS, CHUNK, HEAD_DIM)
    tok_blk = sort_order.reshape(N_CHUNKS, CHUNK)
    key_both = jnp.concatenate([jnp.roll(key_blk, 1, axis=0), key_blk], axis=1)
    val_both = jnp.concatenate([jnp.roll(val_blk, 1, axis=0), val_blk], axis=1)
    tok_both = jnp.concatenate([jnp.roll(tok_blk, 1, axis=0), tok_blk], axis=1)
    logits = jnp.einsum("ncd,nkd->nck", query_blk, key_both) * HEAD_DIM ** -0.5
    logits = jnp.where(tok_blk[:, :, None] == tok_both[:, None, :], MASK_VALUE, logits)
    probs = jax.nn.softmax(logits, axis=-1).astype(jnp.bfloat16).astype(jnp.float32)
    out_sorted = jnp.einsum("nck,nkd->ncd", probs, val_both).astype(jnp.bfloat16)
    return out_sorted.reshape(SEQ_LEN, HEAD_DIM)[sorted_rank]


def reference(hidden, bucket, w_qk, w_v, w_o):
    hidden_wide = hidden.astype(jnp.float32)
    qk_all = jnp.einsum("btd,dhe->bhte", hidden_wide, w_qk.astype(jnp.float32)).astype(jnp.bfloat16)
    v_all = jnp.einsum("btd,dhe->bhte", hidden_wide, w_v.astype(jnp.float32)).astype(jnp.bfloat16)
    positions = jnp.arange(SEQ_LEN, dtype=jnp.int32)
    sort_keys = bucket * SEQ_LEN + positions
    operands = (qk_all.reshape(BATCH * HEADS, SEQ_LEN, HEAD_DIM), v_all.reshape(BATCH * HEADS, SEQ_LEN, HEAD_DIM), sort_keys.reshape(BATCH * HEADS, SEQ_LEN))
    out_heads = lax.map(head_attention, operands)
    attn_out = out_heads.reshape(BATCH, HEADS, SEQ_LEN, HEAD_DIM).astype(jnp.float32)
    return jnp.einsum("bhte,hed->btd", attn_out, w_o.astype(jnp.float32)).astype(jnp.bfloat16)
```

```python
import functools

import jax
import jax.numpy as jnp
from jax import lax
from jax.experimental import pallas as pl
from jax.experimental.pallas import tpu as pltpu
from jax.sharding import PartitionSpec as P

CHIPS = 64
HALF = 32
TOK = 128
CHUNK = 128
HEADS = 16
DIM = 64
MODEL = 2048
SLOTS = 4
MASKED = -8e5
EXP_SCALE = 0.125 * 1.4426950408889634
F32 = jnp.float32
BF16 = jnp.bfloat16
NT = (((1,), (1,)), ((), ()))
TN = (((0,), (0,)), ((), ()))


def iota(shape, axis):
    return lax.broadcasted_iota(jnp.int32, shape, axis)


def one_hot(mask):
    return jnp.where(mask, 1.0, 0.0).astype(BF16)


def dot(a, b, dims=(((1,), (0,)), ((), ()))):
    return lax.dot_general(a, b, dims, preferred_element_type=F32)


def kernel(x_hbm, bucket_ref, wq_hbm, wv_hbm, wo_hbm, y_ref,
           x_buf, w_buf, wo_buf, b_send, b_recv, r_send, r_recv,
           first_rank, code_pair, code_quad, parity, slot_rank,
           slots, slots_out, keys, vals, qrows, back, back_out, o_send, o_recv, part_send, part_recv,
           load_sem, b_send_sem, b_recv_sem, r_send_sem, r_recv_sem, s_send_sem, s_recv_sem,
           k_send_sem, k_recv_sem, o_send_sem, o_recv_sem, p_send_sem, p_recv_sem):
    core = lax.axis_index("tp")
    chip = lax.axis_index("sp")
    other = 1 - core
    half = chip // HALF
    place = chip % HALF
    mine = core == half

    def peer(t, s):
        return {"dp": 0, "tp": t, "sp": s}

    def remote(src, dst, send, recv, t, s):
        return pltpu.make_async_remote_copy(
            src_ref=src, dst_ref=dst, send_sem=send, recv_sem=recv,
            device_id=peer(t, s), device_id_type=pl.DeviceIdType.MESH)

    barrier = pltpu.get_barrier_semaphore()

    def greet(s, _):
        for t in range(2):
            @pl.when((s != chip) | (core != t))
            def _():
                pl.semaphore_signal(barrier, inc=1, device_id=peer(t, s), device_id_type=pl.DeviceIdType.MESH)
        return 0

    lax.fori_loop(0, CHIPS, greet, 0)

    turn = (chip // 8) % 4
    x_load = pltpu.make_async_copy(x_hbm, x_buf, load_sem.at[0])
    x_load.start()

    def w_loads(step):
        group = (step + turn) % 4
        return (pltpu.make_async_copy(wq_hbm.at[pl.ds(group * 256, 256)], w_buf.at[step, 0], load_sem.at[1 + step]),
                pltpu.make_async_copy(wv_hbm.at[pl.ds(group * 256, 256)], w_buf.at[step, 1], load_sem.at[5 + step]))

    for step in range(4):
        for load in w_loads(step):
            load.start()
    wo_load = pltpu.make_async_copy(wo_hbm, wo_buf, load_sem.at[9])
    wo_load.start()

    for b in range(2):
        for h in range(HEADS):
            b_send[b * HEADS + h] = bucket_ref[b, h:h + 1, :]

    x_load.wait()

    def project(step):
        for load in w_loads(step):
            load.wait()
        group = (step + turn) % 4
        rows = dot(w_buf[step].reshape(512, MODEL), x_buf[...], NT).astype(BF16)
        for hh in range(4):
            for b in range(2):
                pair = b * HEADS + group * 4 + hh
                r_send[pair, 0:DIM] = rows[hh * DIM:(hh + 1) * DIM, b * TOK:(b + 1) * TOK]
                r_send[pair, DIM:2 * DIM] = rows[256 + hh * DIM:256 + (hh + 1) * DIM, b * TOK:(b + 1) * TOK]

    def send_rows(step):
        group = (step + turn) % 4

        def body(i, _):
            spot = (i + chip) % 8
            pair = (spot // 4) * HEADS + group * 4 + spot % 4
            target = core * HALF + pair

            @pl.when(target == chip)
            def _():
                @pl.when(mine)
                def _():
                    pltpu.make_async_copy(r_send.at[pair], r_recv.at[place], r_recv_sem.at[place]).start()

            @pl.when((target != chip) | jnp.logical_not(mine))
            def _():
                remote(r_send.at[pair], r_recv.at[place], r_send_sem, r_recv_sem.at[place], half, target).start()
            return 0

        lax.fori_loop(0, 8, body, 0)

    project(0)
    pl.semaphore_wait(barrier, 2 * CHIPS - 1)

    def send_buckets(i, _):
        pair = (i + place) % HALF
        target = core * HALF + pair
        for t in range(2):
            @pl.when((target == chip) & (core == t))
            def _():
                pltpu.make_async_copy(b_send.at[pair], b_recv.at[chip], b_recv_sem).start()

            @pl.when((target != chip) | (core != t))
            def _():
                remote(b_send.at[pair], b_recv.at[chip], b_send_sem, b_recv_sem, t, target).start()
        return 0

    lax.fori_loop(0, HALF, send_buckets, 0)
    send_rows(0)

    def project_more(step, _):
        project(step)
        send_rows(step)
        return 0

    lax.fori_loop(1, 4, project_more, 0)

    pltpu.make_async_copy(b_recv, b_recv, b_recv_sem).wait()
    lane256 = iota((TOK, 256), 1)
    count_mat = one_hot((lane256 >= TOK) | (iota((TOK, 256), 0) < lane256))
    ids = iota((8, CHIPS, TOK), 1)
    ids_f = ids.astype(F32)

    def rank_first(i, running):
        hot = jnp.where(b_recv[pl.ds(8 * i, 8)] == ids, 1.0, 0.0)
        counts = dot(hot.astype(BF16).reshape(512, TOK), count_mat)
        for a in range(8):
            block = counts[a * CHIPS:(a + 1) * CHIPS]
            first_rank[8 * i + a] = jnp.sum(hot[a] * (block[:, :TOK] + running), axis=0, keepdims=True)
            running = running + block[:, TOK:]
        return running

    totals = lax.fori_loop(0, 8, rank_first, jnp.zeros((CHIPS, TOK), F32))
    high = jnp.floor(totals * (1.0 / 64))
    low = totals - 64.0 * high
    below = one_hot(iota((CHIPS, CHIPS), 1) < iota((CHIPS, CHIPS), 0))
    offsets = 64.0 * dot(below, high.astype(BF16)) + dot(below, low.astype(BF16))
    shift = (core * HALF).astype(F32)
    within = iota((8, 1, TOK), 0)
    lane_id = iota((CHIPS, TOK), 1)

    def rank_second(i, chunk_counts):
        hot = jnp.where(b_recv[pl.ds(8 * i, 8)] == ids, 1.0, 0.0)
        rank = first_rank[pl.ds(8 * i, 8)] + jnp.sum(hot * offsets[None], axis=1, keepdims=True)
        chunk = jnp.floor(rank * (1.0 / CHUNK)) - shift
        chunk = jnp.where(chunk < 0.0, chunk + float(CHIPS), chunk)
        hot = jnp.where(chunk == ids_f, 1.0, 0.0)
        counts = dot(hot.astype(BF16).reshape(512, TOK), count_mat)
        slot = jnp.sum(hot * counts[:, :TOK].reshape(8, CHIPS, TOK), axis=1, keepdims=True)
        two = jnp.floor(chunk * 0.5)
        code_pair[pl.ds(8 * i, 8)] = chunk * 8.0 + slot + ((within % 2) * SLOTS).astype(F32)
        code_quad[pl.ds(8 * i, 8)] = two * 16.0 + slot + ((within % 4) * SLOTS).astype(F32)
        parity[pl.ds(8 * i, 8)] = chunk - 2.0 * two
        for a in range(8):
            spot = (8 * i + a + core * HALF) % CHIPS
            chunk_counts = chunk_counts + jnp.where(lane_id == spot, counts[a * CHIPS:(a + 1) * CHIPS, TOK:], 0.0)
        return chunk_counts

    chunk_counts = lax.fori_loop(0, 8, rank_second, jnp.zeros((CHIPS, TOK), F32)).astype(BF16)
    source = iota((TOK, 256), 1) // SLOTS
    sources = iota((TOK, 256), 0)
    base = dot(chunk_counts, one_hot(sources < source))
    filled = dot(chunk_counts, one_hot(sources == source))
    slot_no = (iota((CHIPS, 256), 1) % SLOTS).astype(F32)
    slot_rank[...] = jnp.where(slot_no < filled, base + slot_no, -1.0)

    owner_group = (chip % HEADS) // 4
    ids512 = iota((512, 256), 0).astype(F32)

    def share(quad):
        return remote(slots_out.at[:, quad], slots.at[:, 8 + quad], s_send_sem.at[quad], s_recv_sem.at[quad], other, chip)

    def to_slots(i, _):
        quad = 2 * ((owner_group + 8 - i // 2) % 4) + i % 2
        tiles = []
        for a in range(2):
            spot = quad * 4 + a * 2
            for n in range(2):
                pltpu.make_async_copy(r_recv.at[spot + n], r_recv.at[spot + n], r_recv_sem.at[spot + n]).wait()
            token = core * HALF + spot
            codes = jnp.concatenate([code_pair[token], code_pair[token + 1]], axis=1)
            rows = jnp.concatenate([r_recv[spot], r_recv[spot + 1]], axis=1)
            tiles.append(dot(one_hot(codes == ids512), rows, NT).reshape(CHIPS, 8, TOK))
        tile = jnp.concatenate(tiles, axis=1).astype(BF16)
        slots[1:1 + HALF, quad] = tile[:HALF]
        slots[0, quad] = tile[CHIPS - 1]
        slots_out[1:1 + HALF, quad] = tile[HALF:]
        slots_out[0, quad] = tile[HALF - 1]
        share(quad).start()
        return 0

    lax.fori_loop(0, 8, to_slots, 0)

    def share_wait(quad, _):
        share(quad).wait()
        return 0

    lax.fori_loop(0, 8, share_wait, 0)

    rank_ids = iota((CHUNK, 256), 0).astype(F32)

    def selector(u):
        return one_hot(slot_rank[pl.ds((u + CHIPS - 1) % CHIPS, 1), :] == rank_ids)

    def gather_chunk(u, _):
        rows = dot(selector(u), slots[u].reshape(256, TOK))
        q_wide = rows[:, :DIM]
        inverse = 1.0 / jnp.sqrt(jnp.sum(q_wide * q_wide, axis=1, keepdims=True))
        keys[u] = (q_wide * inverse).astype(BF16)
        qrows[u] = q_wide.astype(BF16)
        vals[u] = rows[:, DIM:].T.astype(BF16)
        return 0

    lax.fori_loop(0, HALF + 1, gather_chunk, 0)
    diagonal = iota((CHUNK, CHUNK), 0) == iota((CHUNK, CHUNK), 1)

    def back_share(n):
        return remote(back_out.at[:, pl.ds(4 * n, 4)], back.at[:, pl.ds(16 + 4 * n, 4)],
                      k_send_sem.at[n], k_recv_sem.at[n], other, chip)

    def attend(n, _):
        outs = []
        for a in range(2):
            u = 2 * n + a + 1
            q = qrows[u]
            before = dot(keys[u - 1], q, NT)
            now = jnp.where(diagonal, MASKED, dot(keys[u], q, NT))
            top = jnp.maximum(jnp.max(before, axis=0, keepdims=True), jnp.max(now, axis=0, keepdims=True))
            before = jnp.exp2((before - top) * EXP_SCALE)
            now = jnp.exp2((now - top) * EXP_SCALE)
            total = jnp.sum(before, axis=0, keepdims=True) + jnp.sum(now, axis=0, keepdims=True)
            inverse = 1.0 / total
            probs = jnp.concatenate([(before * inverse).astype(BF16), (now * inverse).astype(BF16)], axis=0)
            out = dot(jnp.concatenate([vals[u - 1], vals[u]], axis=1), probs).astype(BF16)
            outs.append(dot(out, selector(u)))
        tile = jnp.concatenate(outs, axis=0).T.astype(BF16).reshape(16, 16, TOK)
        back[:, n] = tile[:8]
        back_out[:, n] = tile[8:]

        @pl.when(n % 4 == 3)
        def _():
            back_share(n // 4).start()
        return 0

    lax.fori_loop(0, HALF // 2, attend, 0)

    def back_wait(n, _):
        back_share(n).wait()
        return 0

    lax.fori_loop(0, 4, back_wait, 0)

    ids_quad = iota((512, 512), 0).astype(F32)
    my_pair = place

    def to_tokens(i, _):
        quad = (i + place // 4) % 8
        token = core * HALF + quad * 4
        codes = jnp.concatenate([code_quad[token + a] for a in range(4)], axis=1)
        odd = jnp.concatenate([parity[token + a] for a in range(4)], axis=1)
        both = dot(back[quad].reshape(512, TOK), one_hot(codes == ids_quad), TN)
        rows = jnp.where(odd > 0.5, both[DIM:], both[:DIM]).astype(BF16)
        for a in range(4):
            o_send[quad * 4 + a] = rows[:, a * TOK:(a + 1) * TOK]
        for a in range(4):
            target = token + a

            @pl.when((target == chip) & mine)
            def _():
                pltpu.make_async_copy(o_send.at[quad * 4 + a], o_recv.at[my_pair], o_recv_sem).start()

            @pl.when((target != chip) | jnp.logical_not(mine))
            def _():
                remote(o_send.at[quad * 4 + a], o_recv.at[my_pair], o_send_sem, o_recv_sem, half, target).start()
        return 0

    lax.fori_loop(0, 8, to_tokens, 0)
    wo_load.wait()
    pltpu.make_async_copy(o_recv, o_recv, o_recv_sem).wait()

    def part_share(b):
        return remote(part_send.at[b], part_recv.at[b], p_send_sem.at[b], p_recv_sem.at[b], other, chip)

    def out_rows(b, side):
        lhs = o_recv[pl.ds(b * HEADS, HEADS)].reshape(HEADS * DIM, TOK)
        return dot(lhs, wo_buf[:, pl.ds(pl.multiple_of(side * 1024, 1024), 1024)], TN)

    for b in range(2):
        part_send[b] = out_rows(b, other)
        part_share(b).start()
    mine_parts = [out_rows(b, core) for b in range(2)]
    for b in range(2):
        part_share(b).wait()
        y_ref[b] = (mine_parts[b] + part_recv[b]).astype(BF16)

    @pl.when(mine)
    def _():
        pltpu.make_async_copy(b_recv.at[0:63], b_recv.at[0:63], b_send_sem).wait()
        pltpu.make_async_copy(r_send.at[0:31], r_send.at[0:31], r_send_sem).wait()
        pltpu.make_async_copy(o_send.at[0:31], o_send.at[0:31], o_send_sem).wait()

    @pl.when(jnp.logical_not(mine))
    def _():
        pltpu.make_async_copy(b_recv, b_recv, b_send_sem).wait()
        pltpu.make_async_copy(r_send, r_send, r_send_sem).wait()
        pltpu.make_async_copy(o_send, o_send, o_send_sem).wait()


def solution(mesh):
    def step(hidden, bucket, w_qk, w_v, w_o):
        x = hidden.reshape(2 * TOK, MODEL)
        wq = jnp.transpose(w_qk, (1, 2, 0)).reshape(HEADS * DIM, MODEL)
        wv = jnp.transpose(w_v, (1, 2, 0)).reshape(HEADS * DIM, MODEL)
        wo = w_o.reshape(HEADS * DIM, MODEL)
        any_spec = pl.BlockSpec(memory_space=pl.ANY)
        vmem_spec = pl.BlockSpec(memory_space=pltpu.VMEM)
        dma = pltpu.SemaphoreType.DMA
        return pl.pallas_call(
            kernel,
            out_shape=jax.ShapeDtypeStruct((2, TOK, MODEL // 2), BF16),
            in_specs=[any_spec, vmem_spec, any_spec, any_spec, any_spec],
            out_specs=vmem_spec,
            scratch_shapes=[
                pltpu.VMEM((2 * TOK, MODEL), BF16),
                pltpu.VMEM((4, 2, 256, MODEL), BF16),
                pltpu.VMEM((HEADS * DIM, MODEL), BF16),
                pltpu.VMEM((HALF, 1, TOK), jnp.int32),
                pltpu.VMEM((CHIPS, 1, TOK), jnp.int32),
                pltpu.VMEM((HALF, 2 * DIM, TOK), BF16),
                pltpu.VMEM((HALF, 2 * DIM, TOK), BF16),
                pltpu.VMEM((CHIPS, 1, TOK), F32),
                pltpu.VMEM((CHIPS, 1, TOK), F32),
                pltpu.VMEM((CHIPS, 1, TOK), F32),
                pltpu.VMEM((CHIPS, 1, TOK), F32),
                pltpu.VMEM((CHIPS, 256), F32),
                pltpu.VMEM((HALF + 1, 16, 16, TOK), BF16),
                pltpu.VMEM((HALF + 1, 8, 16, TOK), BF16),
                pltpu.VMEM((HALF + 1, CHUNK, DIM), BF16),
                pltpu.VMEM((HALF + 1, DIM, CHUNK), BF16),
                pltpu.VMEM((HALF + 1, CHUNK, DIM), BF16),
                pltpu.VMEM((8, HALF, 16, TOK), BF16),
                pltpu.VMEM((8, HALF // 2, 16, TOK), BF16),
                pltpu.VMEM((HALF, DIM, TOK), BF16),
                pltpu.VMEM((HALF, DIM, TOK), BF16),
                pltpu.VMEM((2, TOK, MODEL // 2), F32),
                pltpu.VMEM((2, TOK, MODEL // 2), F32),
                dma((10,)), dma(()), dma(()), dma(()), dma((HALF,)), dma((8,)), dma((8,)),
                dma((4,)), dma((4,)), dma(()), dma(()), dma((2,)), dma((2,)),
            ],
            compiler_params=pltpu.CompilerParams(collective_id=0, has_side_effects=True, vmem_limit_bytes=56 * 1024 * 1024),
            name="bucket_attention",
        )(x, bucket, wq, wv, wo)

    return jax.shard_map(
        step, mesh=mesh,
        in_specs=(P("dp", "sp", None), P("dp", "tp", "sp"), P(None, "tp", None), P(None, "tp", None), P("tp", None, None)),
        out_specs=P("dp", "sp", "tp"), check_vma=False)
```

```python
import functools

import jax
import jax.numpy as jnp
from jax import lax
from jax.experimental import pallas as pl
from jax.experimental.pallas import tpu as pltpu
from jax.sharding import PartitionSpec as P

CHIPS = 64
HALF = 32
TOK = 128
CHUNK = 128
HEADS = 16
DIM = 64
MODEL = 2048
SLOTS = 4
MASKED = -8e5
EXP_SCALE = 0.125 * 1.4426950408889634
F32 = jnp.float32
BF16 = jnp.bfloat16
NT = (((1,), (1,)), ((), ()))
TN = (((0,), (0,)), ((), ()))


def iota(shape, axis):
    return lax.broadcasted_iota(jnp.int32, shape, axis)


def one_hot(mask):
    return jnp.where(mask, 1.0, 0.0).astype(BF16)


def dot(a, b, dims=(((1,), (0,)), ((), ()))):
    return lax.dot_general(a, b, dims, preferred_element_type=F32)


def kernel(x_hbm, bucket_ref, wq_hbm, wv_hbm, wo_hbm, y_ref,
           x_buf, w_buf, wo_buf, b_send, b_recv, r_send, r_recv,
           first_rank, code_pair, code_quad, parity, slot_rank,
           slots, slots_out, picks, keys, vals, qrows, back, back_out, o_send, o_recv, part_send, part_recv,
           load_sem, b_send_sem, b_recv_sem, r_send_sem, r_recv_sem, s_send_sem, s_recv_sem,
           k_send_sem, k_recv_sem, o_send_sem, o_recv_sem, p_send_sem, p_recv_sem):
    core = lax.axis_index("tp")
    chip = lax.axis_index("sp")
    other = 1 - core
    half = chip // HALF
    place = chip % HALF
    mine = core == half

    def peer(t, s):
        return {"dp": 0, "tp": t, "sp": s}

    def remote(src, dst, send, recv, t, s):
        return pltpu.make_async_remote_copy(
            src_ref=src, dst_ref=dst, send_sem=send, recv_sem=recv,
            device_id=peer(t, s), device_id_type=pl.DeviceIdType.MESH)

    turn = (chip // 8) % 4
    x_load = pltpu.make_async_copy(x_hbm, x_buf, load_sem.at[0])
    x_load.start()

    def w_loads(step):
        group = (step + turn) % 4
        return (pltpu.make_async_copy(wq_hbm.at[pl.ds(group * 256, 256)], w_buf.at[step, 0], load_sem.at[1 + step]),
                pltpu.make_async_copy(wv_hbm.at[pl.ds(group * 256, 256)], w_buf.at[step, 1], load_sem.at[5 + step]))

    for step in range(4):
        for load in w_loads(step):
            load.start()
    wo_load = pltpu.make_async_copy(wo_hbm, wo_buf, load_sem.at[9])
    wo_load.start()

    barrier = pltpu.get_barrier_semaphore()

    def greet(s, _):
        for t in range(2):
            @pl.when((s != chip) | (core != t))
            def _():
                pl.semaphore_signal(barrier, inc=1, device_id=peer(t, s), device_id_type=pl.DeviceIdType.MESH)
        return 0

    lax.fori_loop(0, CHIPS, greet, 0)

    for b in range(2):
        for h in range(HEADS):
            b_send[b * HEADS + h] = bucket_ref[b, h:h + 1, :]

    x_load.wait()

    def project(step):
        for load in w_loads(step):
            load.wait()
        group = (step + turn) % 4
        rows = dot(w_buf[step].reshape(512, MODEL), x_buf[...], NT).astype(BF16)
        for hh in range(4):
            for b in range(2):
                pair = b * HEADS + group * 4 + hh
                r_send[pair, 0:DIM] = rows[hh * DIM:(hh + 1) * DIM, b * TOK:(b + 1) * TOK]
                r_send[pair, DIM:2 * DIM] = rows[256 + hh * DIM:256 + (hh + 1) * DIM, b * TOK:(b + 1) * TOK]

    def send_rows(step):
        group = (step + turn) % 4

        def body(i, _):
            spot = (i + chip) % 8
            pair = (spot // 4) * HEADS + group * 4 + spot % 4
            target = core * HALF + pair

            @pl.when(target == chip)
            def _():
                @pl.when(mine)
                def _():
                    pltpu.make_async_copy(r_send.at[pair], r_recv.at[place], r_recv_sem.at[place]).start()

            @pl.when((target != chip) | jnp.logical_not(mine))
            def _():
                remote(r_send.at[pair], r_recv.at[place], r_send_sem, r_recv_sem.at[place], half, target).start()
            return 0

        lax.fori_loop(0, 8, body, 0)

    project(0)
    pl.semaphore_wait(barrier, 2 * CHIPS - 1)

    def send_buckets(i, _):
        pair = (i + place) % HALF
        target = core * HALF + pair
        for t in range(2):
            @pl.when((target == chip) & (core == t))
            def _():
                pltpu.make_async_copy(b_send.at[pair], b_recv.at[chip], b_recv_sem).start()

            @pl.when((target != chip) | (core != t))
            def _():
                remote(b_send.at[pair], b_recv.at[chip], b_send_sem, b_recv_sem, t, target).start()
        return 0

    lax.fori_loop(0, HALF, send_buckets, 0)
    send_rows(0)

    def project_more(step, _):
        project(step)
        send_rows(step)
        return 0

    lax.fori_loop(1, 4, project_more, 0)

    pltpu.make_async_copy(b_recv, b_recv, b_recv_sem).wait()
    lane256 = iota((TOK, 256), 1)
    count_mat = one_hot((lane256 >= TOK) | (iota((TOK, 256), 0) < lane256))
    ids = iota((8, CHIPS, TOK), 1)
    ids_f = ids.astype(F32)

    def rank_first(i, running):
        hot = jnp.where(b_recv[pl.ds(8 * i, 8)] == ids, 1.0, 0.0)
        counts = dot(hot.astype(BF16).reshape(512, TOK), count_mat)
        for a in range(8):
            block = counts[a * CHIPS:(a + 1) * CHIPS]
            first_rank[8 * i + a] = jnp.sum(hot[a] * (block[:, :TOK] + running), axis=0, keepdims=True)
            running = running + block[:, TOK:]
        return running

    totals = lax.fori_loop(0, 8, rank_first, jnp.zeros((CHIPS, TOK), F32))
    high = jnp.floor(totals * (1.0 / 64))
    low = totals - 64.0 * high
    below = one_hot(iota((CHIPS, CHIPS), 1) < iota((CHIPS, CHIPS), 0))
    offsets = 64.0 * dot(below, high.astype(BF16)) + dot(below, low.astype(BF16))
    shift = (core * HALF).astype(F32)
    within = iota((8, 1, TOK), 0)
    lane_id = iota((CHIPS, TOK), 1)

    def rank_second(i, chunk_counts):
        hot = jnp.where(b_recv[pl.ds(8 * i, 8)] == ids, 1.0, 0.0)
        rank = first_rank[pl.ds(8 * i, 8)] + jnp.sum(hot * offsets[None], axis=1, keepdims=True)
        chunk = jnp.floor(rank * (1.0 / CHUNK)) - shift
        chunk = jnp.where(chunk < 0.0, chunk + float(CHIPS), chunk)
        hot = jnp.where(chunk == ids_f, 1.0, 0.0)
        counts = dot(hot.astype(BF16).reshape(512, TOK), count_mat)
        slot = jnp.sum(hot * counts[:, :TOK].reshape(8, CHIPS, TOK), axis=1, keepdims=True)
        two = jnp.floor(chunk * 0.5)
        code_pair[pl.ds(8 * i, 8)] = chunk * 8.0 + slot + ((within % 2) * SLOTS).astype(F32)
        code_quad[pl.ds(8 * i, 8)] = two * 16.0 + slot + ((within % 4) * SLOTS).astype(F32)
        parity[pl.ds(8 * i, 8)] = chunk - 2.0 * two
        for a in range(8):
            spot = (8 * i + a + core * HALF) % CHIPS
            chunk_counts = chunk_counts + jnp.where(lane_id == spot, counts[a * CHIPS:(a + 1) * CHIPS, TOK:], 0.0)
        return chunk_counts

    chunk_counts = lax.fori_loop(0, 8, rank_second, jnp.zeros((CHIPS, TOK), F32)).astype(BF16)
    source = iota((TOK, 256), 1) // SLOTS
    sources = iota((TOK, 256), 0)
    base = dot(chunk_counts, one_hot(sources < source))
    filled = dot(chunk_counts, one_hot(sources == source))
    slot_no = (iota((CHIPS, 256), 1) % SLOTS).astype(F32)
    slot_rank[...] = jnp.where(slot_no < filled, base + slot_no, -1.0)

    owner_group = (chip % HEADS) // 4
    ids512 = iota((512, 256), 0).astype(F32)

    def share(quad):
        return remote(slots_out.at[:, quad], slots.at[:, 8 + quad], s_send_sem.at[quad], s_recv_sem.at[quad], other, chip)

    def to_slots(i, _):
        quad = 2 * ((owner_group + 8 - i // 2) % 4) + i % 2
        tiles = []
        for a in range(2):
            spot = quad * 4 + a * 2
            for n in range(2):
                pltpu.make_async_copy(r_recv.at[spot + n], r_recv.at[spot + n], r_recv_sem.at[spot + n]).wait()
            token = core * HALF + spot
            codes = jnp.concatenate([code_pair[token], code_pair[token + 1]], axis=1)
            rows = jnp.concatenate([r_recv[spot], r_recv[spot + 1]], axis=1)
            tiles.append(dot(one_hot(codes == ids512), rows, NT).reshape(CHIPS, 8, TOK))
        tile = jnp.concatenate(tiles, axis=1).astype(BF16)
        slots[1:1 + HALF, quad] = tile[:HALF]
        slots[0, quad] = tile[CHIPS - 1]
        slots_out[1:1 + HALF, quad] = tile[HALF:]
        slots_out[0, quad] = tile[HALF - 1]
        share(quad).start()
        return 0

    lax.fori_loop(0, 8, to_slots, 0)

    def share_wait(quad, _):
        share(quad).wait()
        return 0

    lax.fori_loop(0, 8, share_wait, 0)

    rank_ids = iota((CHUNK, 256), 0).astype(F32)

    def gather_chunks(i, _):
        spots = [3 * i + a for a in range(3)]
        chosen = [one_hot(slot_rank[pl.ds((u + CHIPS - 1) % CHIPS, 1), :] == rank_ids) for u in spots]
        found = [dot(pick, slots[u].reshape(256, TOK)) for u, pick in zip(spots, chosen)]
        for u, pick in zip(spots, chosen):
            picks[u] = pick
        for u, rows in zip(spots, found):
            q_wide = rows[:, :DIM]
            inverse = 1.0 / jnp.sqrt(jnp.sum(q_wide * q_wide, axis=1, keepdims=True))
            keys[u] = (q_wide * inverse).astype(BF16)
            qrows[u] = q_wide.astype(BF16)
            vals[u] = rows[:, DIM:].T.astype(BF16)
        return 0

    lax.fori_loop(0, (HALF + 1) // 3, gather_chunks, 0)
    diagonal = iota((CHUNK, CHUNK), 0) == iota((CHUNK, CHUNK), 1)

    def back_share(n):
        return remote(back_out.at[:, pl.ds(4 * n, 4)], back.at[:, pl.ds(16 + 4 * n, 4)],
                      k_send_sem.at[n], k_recv_sem.at[n], other, chip)

    def softmax(before, now):
        now = jnp.where(diagonal, MASKED, now)
        top = jnp.maximum(jnp.max(before, axis=0, keepdims=True), jnp.max(now, axis=0, keepdims=True))
        before = jnp.exp2((before - top) * EXP_SCALE)
        now = jnp.exp2((now - top) * EXP_SCALE)
        total = jnp.sum(before, axis=0, keepdims=True) + jnp.sum(now, axis=0, keepdims=True)
        inverse = 1.0 / total
        return jnp.concatenate([(before * inverse).astype(BF16), (now * inverse).astype(BF16)], axis=0)

    def attend(n, _):
        spots = [4 * n + a + 1 for a in range(4)]
        scores = [(dot(keys[u - 1], qrows[u], NT), dot(keys[u], qrows[u], NT)) for u in spots]
        probs = [softmax(*pair) for pair in scores]
        outs = [dot(jnp.concatenate([vals[u - 1], vals[u]], axis=1), p).astype(BF16) for u, p in zip(spots, probs)]
        spread = [dot(o, picks[u]) for u, o in zip(spots, outs)]
        for m in range(2):
            tile = jnp.concatenate(spread[2 * m:2 * m + 2], axis=0).T.astype(BF16).reshape(16, 16, TOK)
            back[:, 2 * n + m] = tile[:8]
            back_out[:, 2 * n + m] = tile[8:]

        @pl.when(n % 2 == 1)
        def _():
            back_share(n // 2).start()
        return 0

    lax.fori_loop(0, HALF // 4, attend, 0)

    def back_wait(n, _):
        back_share(n).wait()
        return 0

    lax.fori_loop(0, 4, back_wait, 0)

    ids_quad = iota((512, 512), 0).astype(F32)
    my_pair = place

    def to_tokens(i, _):
        quad = (i + place // 4) % 8
        token = core * HALF + quad * 4
        codes = jnp.concatenate([code_quad[token + a] for a in range(4)], axis=1)
        odd = jnp.concatenate([parity[token + a] for a in range(4)], axis=1)
        both = dot(back[quad].reshape(512, TOK), one_hot(codes == ids_quad), TN)
        rows = jnp.where(odd > 0.5, both[DIM:], both[:DIM]).astype(BF16)
        for a in range(4):
            o_send[quad * 4 + a] = rows[:, a * TOK:(a + 1) * TOK]
        for a in range(4):
            target = token + a

            @pl.when((target == chip) & mine)
            def _():
                pltpu.make_async_copy(o_send.at[quad * 4 + a], o_recv.at[my_pair], o_recv_sem).start()

            @pl.when((target != chip) | jnp.logical_not(mine))
            def _():
                remote(o_send.at[quad * 4 + a], o_recv.at[my_pair], o_send_sem, o_recv_sem, half, target).start()
        return 0

    lax.fori_loop(0, 8, to_tokens, 0)
    wo_load.wait()
    pltpu.make_async_copy(o_recv, o_recv, o_recv_sem).wait()

    def part_share(b):
        return remote(part_send.at[b], part_recv.at[b], p_send_sem.at[b], p_recv_sem.at[b], other, chip)

    def out_rows(b, side):
        lhs = o_recv[pl.ds(b * HEADS, HEADS)].reshape(HEADS * DIM, TOK)
        return dot(lhs, wo_buf[:, pl.ds(pl.multiple_of(side * 1024, 1024), 1024)], TN)

    for b in range(2):
        part_send[b] = out_rows(b, other)
        part_share(b).start()
    mine_parts = [out_rows(b, core) for b in range(2)]
    for b in range(2):
        part_share(b).wait()
        y_ref[b] = (mine_parts[b] + part_recv[b]).astype(BF16)

    @pl.when(mine)
    def _():
        pltpu.make_async_copy(b_recv.at[0:63], b_recv.at[0:63], b_send_sem).wait()
        pltpu.make_async_copy(r_send.at[0:31], r_send.at[0:31], r_send_sem).wait()
        pltpu.make_async_copy(o_send.at[0:31], o_send.at[0:31], o_send_sem).wait()

    @pl.when(jnp.logical_not(mine))
    def _():
        pltpu.make_async_copy(b_recv, b_recv, b_send_sem).wait()
        pltpu.make_async_copy(r_send, r_send, r_send_sem).wait()
        pltpu.make_async_copy(o_send, o_send, o_send_sem).wait()


def solution(mesh):
    def step(hidden, bucket, w_qk, w_v, w_o):
        x = hidden.reshape(2 * TOK, MODEL)
        wq = jnp.transpose(w_qk, (1, 2, 0)).reshape(HEADS * DIM, MODEL)
        wv = jnp.transpose(w_v, (1, 2, 0)).reshape(HEADS * DIM, MODEL)
        wo = w_o.reshape(HEADS * DIM, MODEL)
        any_spec = pl.BlockSpec(memory_space=pl.ANY)
        vmem_spec = pl.BlockSpec(memory_space=pltpu.VMEM)
        dma = pltpu.SemaphoreType.DMA
        return pl.pallas_call(
            kernel,
            out_shape=jax.ShapeDtypeStruct((2, TOK, MODEL // 2), BF16),
            in_specs=[any_spec, vmem_spec, any_spec, any_spec, any_spec],
            out_specs=vmem_spec,
            scratch_shapes=[
                pltpu.VMEM((2 * TOK, MODEL), BF16),
                pltpu.VMEM((4, 2, 256, MODEL), BF16),
                pltpu.VMEM((HEADS * DIM, MODEL), BF16),
                pltpu.VMEM((HALF, 1, TOK), jnp.int32),
                pltpu.VMEM((CHIPS, 1, TOK), jnp.int32),
                pltpu.VMEM((HALF, 2 * DIM, TOK), BF16),
                pltpu.VMEM((HALF, 2 * DIM, TOK), BF16),
                pltpu.VMEM((CHIPS, 1, TOK), F32),
                pltpu.VMEM((CHIPS, 1, TOK), F32),
                pltpu.VMEM((CHIPS, 1, TOK), F32),
                pltpu.VMEM((CHIPS, 1, TOK), F32),
                pltpu.VMEM((CHIPS, 256), F32),
                pltpu.VMEM((HALF + 1, 16, 16, TOK), BF16),
                pltpu.VMEM((HALF + 1, 8, 16, TOK), BF16),
                pltpu.VMEM((HALF + 1, CHUNK, 256), BF16),
                pltpu.VMEM((HALF + 1, CHUNK, DIM), BF16),
                pltpu.VMEM((HALF + 1, DIM, CHUNK), BF16),
                pltpu.VMEM((HALF + 1, CHUNK, DIM), BF16),
                pltpu.VMEM((8, HALF, 16, TOK), BF16),
                pltpu.VMEM((8, HALF // 2, 16, TOK), BF16),
                pltpu.VMEM((HALF, DIM, TOK), BF16),
                pltpu.VMEM((HALF, DIM, TOK), BF16),
                pltpu.VMEM((2, TOK, MODEL // 2), F32),
                pltpu.VMEM((2, TOK, MODEL // 2), F32),
                dma((10,)), dma(()), dma(()), dma(()), dma((HALF,)), dma((8,)), dma((8,)),
                dma((4,)), dma((4,)), dma(()), dma(()), dma((2,)), dma((2,)),
            ],
            compiler_params=pltpu.CompilerParams(collective_id=0, has_side_effects=True, vmem_limit_bytes=56 * 1024 * 1024),
            name="bucket_attention",
        )(x, bucket, wq, wv, wo)

    return jax.shard_map(
        step, mesh=mesh,
        in_specs=(P("dp", "sp", None), P("dp", "tp", "sp"), P(None, "tp", None), P(None, "tp", None), P("tp", None, None)),
        out_specs=P("dp", "sp", "tp"), check_vma=False)
```

```python
import functools

import jax
import jax.numpy as jnp
from jax import lax
from jax.experimental import pallas as pl
from jax.experimental.pallas import tpu as pltpu
from jax.sharding import PartitionSpec as P

CHIPS = 64
HALF = 32
TOK = 128
CHUNK = 128
HEADS = 16
DIM = 64
MODEL = 2048
SLOTS = 4
MASKED = -8e5
EXP_SCALE = 0.125 * 1.4426950408889634
F32 = jnp.float32
BF16 = jnp.bfloat16
NT = (((1,), (1,)), ((), ()))
TN = (((0,), (0,)), ((), ()))


def iota(shape, axis):
    return lax.broadcasted_iota(jnp.int32, shape, axis)


def one_hot(mask):
    return jnp.where(mask, 1.0, 0.0).astype(BF16)


def dot(a, b, dims=(((1,), (0,)), ((), ()))):
    return lax.dot_general(a, b, dims, preferred_element_type=F32)


def kernel(x_hbm, bucket_ref, wq_hbm, wv_hbm, wo_hbm, y_ref,
           x_buf, w_buf, wo_buf, b_send, b_recv, r_send, r_recv,
           first_rank, code_pair, code_quad, parity, slot_rank,
           slots, slots_out, picks, keys, vals, qrows, back, back_out, o_send, o_recv, acc, part_recv,
           load_sem, b_send_sem, b_recv_sem, r_send_sem, r_recv_sem, s_send_sem, s_recv_sem,
           k_send_sem, k_recv_sem, o_send_sem, o_recv_sem, p_send_sem, p_recv_sem):
    core = lax.axis_index("tp")
    chip = lax.axis_index("sp")
    other = 1 - core
    half = chip // HALF
    place = chip % HALF
    mine = core == half

    def peer(t, s):
        return {"dp": 0, "tp": t, "sp": s}

    def remote(src, dst, send, recv, t, s):
        return pltpu.make_async_remote_copy(
            src_ref=src, dst_ref=dst, send_sem=send, recv_sem=recv,
            device_id=peer(t, s), device_id_type=pl.DeviceIdType.MESH)

    turn = (chip // 8) % 4
    x_load = pltpu.make_async_copy(x_hbm, x_buf, load_sem.at[0])
    x_load.start()

    def w_loads(step):
        group = (step + turn) % 4
        return (pltpu.make_async_copy(wq_hbm.at[pl.ds(group * 256, 256)], w_buf.at[step, 0], load_sem.at[1 + step]),
                pltpu.make_async_copy(wv_hbm.at[pl.ds(group * 256, 256)], w_buf.at[step, 1], load_sem.at[5 + step]))

    for step in range(4):
        for load in w_loads(step):
            load.start()
    wo_loads = [pltpu.make_async_copy(wo_hbm.at[g], wo_buf.at[g], load_sem.at[9 + g]) for g in range(4)]
    for load in wo_loads:
        load.start()

    barrier = pltpu.get_barrier_semaphore()

    def greet(s, _):
        for t in range(2):
            @pl.when((s != chip) | (core != t))
            def _():
                pl.semaphore_signal(barrier, inc=1, device_id=peer(t, s), device_id_type=pl.DeviceIdType.MESH)
        return 0

    lax.fori_loop(0, CHIPS, greet, 0)

    for b in range(2):
        for h in range(HEADS):
            b_send[b * HEADS + h] = bucket_ref[b, h:h + 1, :]

    x_load.wait()

    def project(step):
        for load in w_loads(step):
            load.wait()
        group = (step + turn) % 4
        rows = dot(w_buf[step].reshape(512, MODEL), x_buf[...], NT).astype(BF16)
        for hh in range(4):
            for b in range(2):
                pair = b * HEADS + group * 4 + hh
                r_send[pair, 0:DIM] = rows[hh * DIM:(hh + 1) * DIM, b * TOK:(b + 1) * TOK]
                r_send[pair, DIM:2 * DIM] = rows[256 + hh * DIM:256 + (hh + 1) * DIM, b * TOK:(b + 1) * TOK]

    def send_rows(step):
        group = (step + turn) % 4

        def body(i, _):
            spot = (i + chip // 4 + chip // 16) % 8
            pair = (spot // 4) * HEADS + group * 4 + spot % 4
            target = core * HALF + (spot // 4) * HEADS + (spot % 4) * 4 + group

            @pl.when((target == chip) & mine)
            def _():
                pltpu.make_async_copy(r_send.at[pair], r_recv.at[place], r_recv_sem.at[place]).start()

            @pl.when((target != chip) | jnp.logical_not(mine))
            def _():
                remote(r_send.at[pair], r_recv.at[place], r_send_sem, r_recv_sem.at[place], half, target).start()
            return 0

        lax.fori_loop(0, 8, body, 0)

    def send_buckets(i, _):
        spot = (i + place) % HALF
        pair = (spot // HEADS) * HEADS + (spot % 4) * 4 + (spot // 4) % 4
        target = core * HALF + spot
        for t in range(2):
            @pl.when((target == chip) & (core == t))
            def _():
                pltpu.make_async_copy(b_send.at[pair], b_recv.at[chip], b_recv_sem).start()

            @pl.when((target != chip) | (core != t))
            def _():
                remote(b_send.at[pair], b_recv.at[chip], b_send_sem, b_recv_sem, t, target).start()
        return 0

    project(0)
    project(1)
    acc[...] = jnp.zeros_like(acc)
    pl.semaphore_wait(barrier, 2 * CHIPS - 1)
    lax.fori_loop(0, HALF, send_buckets, 0)
    send_rows(0)
    send_rows(1)

    def project_more(step, _):
        project(step)
        send_rows(step)
        return 0

    lax.fori_loop(2, 4, project_more, 0)

    pltpu.make_async_copy(b_recv, b_recv, b_recv_sem).wait()
    lane256 = iota((TOK, 256), 1)
    count_mat = one_hot((lane256 >= TOK) | (iota((TOK, 256), 0) < lane256))
    ids = iota((8, CHIPS, TOK), 1)
    ids_f = ids.astype(F32)

    def rank_first(i, running):
        hot = jnp.where(b_recv[pl.ds(8 * i, 8)] == ids, 1.0, 0.0)
        counts = dot(hot.astype(BF16).reshape(512, TOK), count_mat)
        for a in range(8):
            block = counts[a * CHIPS:(a + 1) * CHIPS]
            first_rank[8 * i + a] = jnp.sum(hot[a] * (block[:, :TOK] + running), axis=0, keepdims=True)
            running = running + block[:, TOK:]
        return running

    totals = lax.fori_loop(0, 8, rank_first, jnp.zeros((CHIPS, TOK), F32))
    high = jnp.floor(totals * (1.0 / 64))
    low = totals - 64.0 * high
    below = one_hot(iota((CHIPS, CHIPS), 1) < iota((CHIPS, CHIPS), 0))
    offsets = 64.0 * dot(below, high.astype(BF16)) + dot(below, low.astype(BF16))
    shift = (core * HALF).astype(F32)
    within = iota((8, 1, TOK), 0)
    lane_id = iota((CHIPS, TOK), 1)

    def rank_second(i, chunk_counts):
        hot = jnp.where(b_recv[pl.ds(8 * i, 8)] == ids, 1.0, 0.0)
        rank = first_rank[pl.ds(8 * i, 8)] + jnp.sum(hot * offsets[None], axis=1, keepdims=True)
        chunk = jnp.floor(rank * (1.0 / CHUNK)) - shift
        chunk = jnp.where(chunk < 0.0, chunk + float(CHIPS), chunk)
        hot = jnp.where(chunk == ids_f, 1.0, 0.0)
        counts = dot(hot.astype(BF16).reshape(512, TOK), count_mat)
        slot = jnp.sum(hot * counts[:, :TOK].reshape(8, CHIPS, TOK), axis=1, keepdims=True)
        two = jnp.floor(chunk * 0.5)
        code_pair[pl.ds(8 * i, 8)] = chunk * 8.0 + slot + ((within % 2) * SLOTS).astype(F32)
        code_quad[pl.ds(8 * i, 8)] = two * 16.0 + slot + ((within % 4) * SLOTS).astype(F32)
        parity[pl.ds(8 * i, 8)] = chunk - 2.0 * two
        for a in range(8):
            spot = (8 * i + a + core * HALF) % CHIPS
            chunk_counts = chunk_counts + jnp.where(lane_id == spot, counts[a * CHIPS:(a + 1) * CHIPS, TOK:], 0.0)
        return chunk_counts

    chunk_counts = lax.fori_loop(0, 8, rank_second, jnp.zeros((CHIPS, TOK), F32)).astype(BF16)
    source = iota((TOK, 256), 1) // SLOTS
    sources = iota((TOK, 256), 0)
    base = dot(chunk_counts, one_hot(sources < source))
    filled = dot(chunk_counts, one_hot(sources == source))
    slot_no = (iota((CHIPS, 256), 1) % SLOTS).astype(F32)
    slot_rank[...] = jnp.where(slot_no < filled, base + slot_no, -1.0)

    owner_group = chip % 4
    ids512 = iota((512, 256), 0).astype(F32)

    def share(quad):
        return remote(slots_out.at[:, quad], slots.at[:, 8 + quad], s_send_sem.at[quad], s_recv_sem.at[quad], other, chip)

    def to_slots(i, _):
        quad = 2 * ((owner_group + 8 - i // 2) % 4) + i % 2
        tiles = []
        for a in range(2):
            spot = quad * 4 + a * 2
            for n in range(2):
                pltpu.make_async_copy(r_recv.at[spot + n], r_recv.at[spot + n], r_recv_sem.at[spot + n]).wait()
            token = core * HALF + spot
            codes = jnp.concatenate([code_pair[token], code_pair[token + 1]], axis=1)
            rows = jnp.concatenate([r_recv[spot], r_recv[spot + 1]], axis=1)
            tiles.append(dot(one_hot(codes == ids512), rows, NT).reshape(CHIPS, 8, TOK))
        tile = jnp.concatenate(tiles, axis=1).astype(BF16)
        slots[1:1 + HALF, quad] = tile[:HALF]
        slots[0, quad] = tile[CHIPS - 1]
        slots_out[1:1 + HALF, quad] = tile[HALF:]
        slots_out[0, quad] = tile[HALF - 1]
        share(quad).start()
        return 0

    lax.fori_loop(0, 8, to_slots, 0)

    def share_wait(quad, _):
        share(quad).wait()
        return 0

    lax.fori_loop(0, 8, share_wait, 0)

    rank_ids = iota((CHUNK, 256), 0).astype(F32)

    def gather_chunks(i, _):
        spots = [11 * i + a for a in range(11)]
        chosen = [one_hot(slot_rank[pl.ds((u + CHIPS - 1) % CHIPS, 1), :] == rank_ids) for u in spots]
        found = [dot(pick, slots[u].reshape(256, TOK)) for u, pick in zip(spots, chosen)]
        for u, pick in zip(spots, chosen):
            picks[u] = pick
        for u, rows in zip(spots, found):
            q_wide = rows[:, :DIM]
            inverse = 1.0 / jnp.sqrt(jnp.sum(q_wide * q_wide, axis=1, keepdims=True))
            keys[u] = (q_wide * inverse).astype(BF16)
            qrows[u] = q_wide.astype(BF16)
            vals[u] = rows[:, DIM:].T.astype(BF16)
        return 0

    lax.fori_loop(0, (HALF + 1) // 11, gather_chunks, 0)
    diagonal = iota((CHUNK, CHUNK), 0) == iota((CHUNK, CHUNK), 1)

    def back_share(n):
        return remote(back_out.at[:, pl.ds(4 * n, 4)], back.at[:, pl.ds(16 + 4 * n, 4)],
                      k_send_sem.at[n], k_recv_sem.at[n], other, chip)

    def softmax(both):
        before, now = both[:CHUNK], jnp.where(diagonal, MASKED, both[CHUNK:])
        top = jnp.maximum(jnp.max(before, axis=0, keepdims=True), jnp.max(now, axis=0, keepdims=True))
        before = jnp.exp2((before - top) * EXP_SCALE)
        now = jnp.exp2((now - top) * EXP_SCALE)
        total = jnp.sum(before, axis=0, keepdims=True) + jnp.sum(now, axis=0, keepdims=True)
        inverse = 1.0 / total
        return jnp.concatenate([(before * inverse).astype(BF16), (now * inverse).astype(BF16)], axis=0)

    def attend(n, _):
        spots = [8 * n + a + 1 for a in range(8)]
        scores = [dot(keys[pl.ds(u - 1, 2)].reshape(2 * CHUNK, DIM), qrows[u], NT) for u in spots]
        probs = [softmax(both) for both in scores]
        outs = [dot(jnp.concatenate([vals[u - 1], vals[u]], axis=1), p).astype(BF16) for u, p in zip(spots, probs)]
        spread = [dot(o, picks[u]) for u, o in zip(spots, outs)]
        for m in range(4):
            tile = jnp.concatenate(spread[2 * m:2 * m + 2], axis=0).T.astype(BF16).reshape(16, 16, TOK)
            back[:, 4 * n + m] = tile[:8]
            back_out[:, 4 * n + m] = tile[8:]

        back_share(n).start()
        return 0

    lax.fori_loop(0, HALF // 8, attend, 0)

    def back_wait(n, _):
        back_share(n).wait()
        return 0

    lax.fori_loop(0, 4, back_wait, 0)

    ids_quad = iota((512, 512), 0).astype(F32)
    my_batch = place // HEADS
    my_pair = my_batch * HEADS + (chip % 4) * 4 + (chip // 4) % 4

    def to_tokens(i, _):
        quad = (((i // 4) + my_batch) % 2) * 4 + (i + chip) % 4
        token = core * HALF + quad * 4
        codes = jnp.concatenate([code_quad[token + a] for a in range(4)], axis=1)
        odd = jnp.concatenate([parity[token + a] for a in range(4)], axis=1)
        both = dot(back[quad].reshape(512, TOK), one_hot(codes == ids_quad), TN)
        rows = jnp.where(odd > 0.5, both[DIM:], both[:DIM]).astype(BF16)
        for a in range(4):
            o_send[quad * 4 + a] = rows[:, a * TOK:(a + 1) * TOK]
        for n in range(4):
            a = (n + chip // 4 + chip // 16) % 4
            target = token + a

            @pl.when((target == chip) & mine)
            def _():
                pltpu.make_async_copy(o_send.at[quad * 4 + a], o_recv.at[my_pair], o_recv_sem.at[my_pair]).start()

            @pl.when((target != chip) | jnp.logical_not(mine))
            def _():
                remote(o_send.at[quad * 4 + a], o_recv.at[my_pair], o_send_sem, o_recv_sem.at[my_pair], half, target).start()
        return 0

    lax.fori_loop(0, 8, to_tokens, 0)
    for load in wo_loads:
        load.wait()

    def part_share(b):
        return remote(acc.at[b, other], part_recv.at[b], p_send_sem.at[b], p_recv_sem.at[b], other, chip)

    my_quad = place // 4

    def project_out(i, _):
        b = (i // 4 + my_quad // 4) % 2
        group = (my_quad + 4 - i % 4) % 4
        first = b * HEADS + group * 4
        for n in range(4):
            pltpu.make_async_copy(o_recv.at[first + n], o_recv.at[first + n], o_recv_sem.at[first + n]).wait()
        lhs = o_recv[pl.ds(first, 4)].reshape(256, TOK)
        for side in range(2):
            acc[b, side] += dot(lhs, wo_buf[group, :, side * 1024:(side + 1) * 1024], TN)

        @pl.when(i % 4 == 3)
        def _():
            part_share(b).start()
        return 0

    lax.fori_loop(0, 8, project_out, 0)

    def finish(n, _):
        b = (n + my_quad // 4) % 2
        part_share(b).wait()
        y_ref[b] = (acc[b, core] + part_recv[b]).astype(BF16)
        return 0

    lax.fori_loop(0, 2, finish, 0)

    @pl.when(mine)
    def _():
        pltpu.make_async_copy(b_recv.at[0:63], b_recv.at[0:63], b_send_sem).wait()
        pltpu.make_async_copy(r_send.at[0:31], r_send.at[0:31], r_send_sem).wait()
        pltpu.make_async_copy(o_send.at[0:31], o_send.at[0:31], o_send_sem).wait()

    @pl.when(jnp.logical_not(mine))
    def _():
        pltpu.make_async_copy(b_recv, b_recv, b_send_sem).wait()
        pltpu.make_async_copy(r_send, r_send, r_send_sem).wait()
        pltpu.make_async_copy(o_send, o_send, o_send_sem).wait()


def solution(mesh):
    def step(hidden, bucket, w_qk, w_v, w_o):
        x = hidden.reshape(2 * TOK, MODEL)
        wq = jnp.transpose(w_qk, (1, 2, 0)).reshape(HEADS * DIM, MODEL)
        wv = jnp.transpose(w_v, (1, 2, 0)).reshape(HEADS * DIM, MODEL)
        wo = w_o.reshape(4, 256, MODEL)
        any_spec = pl.BlockSpec(memory_space=pl.ANY)
        vmem_spec = pl.BlockSpec(memory_space=pltpu.VMEM)
        dma = pltpu.SemaphoreType.DMA
        return pl.pallas_call(
            kernel,
            out_shape=jax.ShapeDtypeStruct((2, TOK, MODEL // 2), BF16),
            in_specs=[any_spec, vmem_spec, any_spec, any_spec, any_spec],
            out_specs=vmem_spec,
            scratch_shapes=[
                pltpu.VMEM((2 * TOK, MODEL), BF16),
                pltpu.VMEM((4, 2, 256, MODEL), BF16),
                pltpu.VMEM((4, 256, MODEL), BF16),
                pltpu.VMEM((HALF, 1, TOK), jnp.int32),
                pltpu.VMEM((CHIPS, 1, TOK), jnp.int32),
                pltpu.VMEM((HALF, 2 * DIM, TOK), BF16),
                pltpu.VMEM((HALF, 2 * DIM, TOK), BF16),
                pltpu.VMEM((CHIPS, 1, TOK), F32),
                pltpu.VMEM((CHIPS, 1, TOK), F32),
                pltpu.VMEM((CHIPS, 1, TOK), F32),
                pltpu.VMEM((CHIPS, 1, TOK), F32),
                pltpu.VMEM((CHIPS, 256), F32),
                pltpu.VMEM((HALF + 1, 16, 16, TOK), BF16),
                pltpu.VMEM((HALF + 1, 8, 16, TOK), BF16),
                pltpu.VMEM((HALF + 1, CHUNK, 256), BF16),
                pltpu.VMEM((HALF + 1, CHUNK, DIM), BF16),
                pltpu.VMEM((HALF + 1, DIM, CHUNK), BF16),
                pltpu.VMEM((HALF + 1, CHUNK, DIM), BF16),
                pltpu.VMEM((8, HALF, 16, TOK), BF16),
                pltpu.VMEM((8, HALF // 2, 16, TOK), BF16),
                pltpu.VMEM((HALF, DIM, TOK), BF16),
                pltpu.VMEM((HALF, DIM, TOK), BF16),
                pltpu.VMEM((2, 2, TOK, MODEL // 2), F32),
                pltpu.VMEM((2, TOK, MODEL // 2), F32),
                dma((13,)), dma(()), dma(()), dma(()), dma((HALF,)), dma((8,)), dma((8,)),
                dma((4,)), dma((4,)), dma(()), dma((HALF,)), dma((2,)), dma((2,)),
            ],
            compiler_params=pltpu.CompilerParams(collective_id=0, has_side_effects=True, vmem_limit_bytes=56 * 1024 * 1024),
            name="bucket_attention",
        )(x, bucket, wq, wv, wo)

    return jax.shard_map(
        step, mesh=mesh,
        in_specs=(P("dp", "sp", None), P("dp", "tp", "sp"), P(None, "tp", None), P(None, "tp", None), P("tp", None, None)),
        out_specs=P("dp", "sp", "tp"), check_vma=False)
```

```python
import functools

import jax
import jax.numpy as jnp
from jax import lax
from jax.experimental import pallas as pl
from jax.experimental.pallas import tpu as pltpu
from jax.sharding import PartitionSpec as P

CHIPS = 64
HALF = 32
TOK = 128
CHUNK = 128
HEADS = 16
DIM = 64
MODEL = 2048
SLOTS = 4
MASKED = -8e5
EXP_SCALE = 0.125 * 1.4426950408889634
F32 = jnp.float32
BF16 = jnp.bfloat16
NT = (((1,), (1,)), ((), ()))
TN = (((0,), (0,)), ((), ()))


def iota(shape, axis):
    return lax.broadcasted_iota(jnp.int32, shape, axis)


def one_hot(mask):
    return jnp.where(mask, 1.0, 0.0).astype(BF16)


def dot(a, b, dims=(((1,), (0,)), ((), ()))):
    return lax.dot_general(a, b, dims, preferred_element_type=F32)


def kernel(x_hbm, bucket_ref, wq_hbm, wv_hbm, wo_hbm, y_ref,
           x_buf, w_buf, wo_buf, b_send, b_recv, r_send, r_recv,
           first_rank, code_pair, code_quad, parity, slot_rank,
           slots, slots_out, picks, token_hot, found_own, token_own, keys, vals, qrows, back, back_out, o_send, o_recv, acc, part_recv,
           load_sem, b_send_sem, b_recv_sem, b_pass_sem, r_send_sem, r_recv_sem, s_send_sem, s_recv_sem,
           k_send_sem, k_recv_sem, o_send_sem, o_recv_sem, p_send_sem, p_recv_sem):
    core = lax.axis_index("tp")
    chip = lax.axis_index("sp")
    other = 1 - core
    half = chip // HALF
    place = chip % HALF
    mine = core == half

    def peer(t, s):
        return {"dp": 0, "tp": t, "sp": s}

    def remote(src, dst, send, recv, t, s):
        return pltpu.make_async_remote_copy(
            src_ref=src, dst_ref=dst, send_sem=send, recv_sem=recv,
            device_id=peer(t, s), device_id_type=pl.DeviceIdType.MESH)

    turn = (chip // 8) % 4
    x_load = pltpu.make_async_copy(x_hbm, x_buf, load_sem.at[0])
    x_load.start()

    def w_loads(step):
        group = (step + turn) % 4
        return (pltpu.make_async_copy(wq_hbm.at[pl.ds(group * 256, 256)], w_buf.at[step, 0], load_sem.at[1 + step]),
                pltpu.make_async_copy(wv_hbm.at[pl.ds(group * 256, 256)], w_buf.at[step, 1], load_sem.at[5 + step]))

    for step in range(4):
        for load in w_loads(step):
            load.start()
    wo_loads = [pltpu.make_async_copy(wo_hbm.at[g], wo_buf.at[g], load_sem.at[9 + g]) for g in range(4)]
    for load in wo_loads:
        load.start()

    barrier = pltpu.get_barrier_semaphore()

    def greet(t, s):
        pl.semaphore_signal(barrier, inc=1, device_id=peer(t, s), device_id_type=pl.DeviceIdType.MESH)

    def greet_chip(i, _):
        spot = (place + i) % HALF
        greet(0, core * HALF + spot)
        greet(1, core * HALF + spot)
        greet(half, other * HALF + spot)
        return 0

    lax.fori_loop(1, HALF, greet_chip, 0)
    greet(half, other * HALF + place)
    greet(1 - half, core * HALF + place)

    @pl.when(jnp.logical_not(mine))
    def _():
        greet(half, core * HALF + place)

    for b in range(2):
        for h in range(HEADS):
            b_send[b * HEADS + h] = bucket_ref[b, h:h + 1, :]

    x_load.wait()

    def project(step):
        for load in w_loads(step):
            load.wait()
        group = (step + turn) % 4
        rows = dot(w_buf[step].reshape(512, MODEL), x_buf[...], NT).astype(BF16)
        for hh in range(4):
            for b in range(2):
                pair = b * HEADS + group * 4 + hh
                r_send[pair, 0:DIM] = rows[hh * DIM:(hh + 1) * DIM, b * TOK:(b + 1) * TOK]
                r_send[pair, DIM:2 * DIM] = rows[256 + hh * DIM:256 + (hh + 1) * DIM, b * TOK:(b + 1) * TOK]

    def send_rows(step):
        group = (step + turn) % 4

        def body(i, _):
            spot = (i + chip // 4 + chip // 16) % 8
            pair = (spot // 4) * HEADS + group * 4 + spot % 4
            target = core * HALF + (spot // 4) * HEADS + (spot % 4) * 4 + group

            @pl.when((target == chip) & mine)
            def _():
                pltpu.make_async_copy(r_send.at[pair], r_recv.at[place], r_recv_sem.at[place]).start()

            @pl.when((target != chip) | jnp.logical_not(mine))
            def _():
                remote(r_send.at[pair], r_recv.at[place], r_send_sem, r_recv_sem.at[place], half, target).start()
            return 0

        lax.fori_loop(0, 8, body, 0)

    def send_buckets(i, _):
        spot = (i + place) % HALF
        pair = (spot // HEADS) * HEADS + (spot % 4) * 4 + (spot // 4) % 4
        target = core * HALF + spot

        @pl.when((i == 0) & mine)
        def _():
            pltpu.make_async_copy(b_send.at[pair], b_recv.at[chip], b_recv_sem).start()

        @pl.when((i > 0) | jnp.logical_not(mine))
        def _():
            remote(b_send.at[pair], b_recv.at[chip], b_send_sem, b_recv_sem, half, target).start()
        return 0

    project(0)
    project(1)
    acc[...] = jnp.zeros_like(acc)
    @pl.when(mine)
    def _():
        pl.semaphore_wait(barrier, 95)

    @pl.when(jnp.logical_not(mine))
    def _():
        pl.semaphore_wait(barrier, 96)

    lax.fori_loop(0, HALF, send_buckets, 0)
    send_rows(0)
    send_rows(1)

    def project_more(step, _):
        project(step)
        send_rows(step)
        return 0

    lax.fori_loop(2, 4, project_more, 0)

    own_rows = b_recv.at[pl.ds(core * HALF, HALF)]
    pltpu.make_async_copy(own_rows, own_rows, b_recv_sem).wait()
    bucket_share = remote(own_rows, own_rows, b_pass_sem.at[0], b_pass_sem.at[1], other, chip)
    bucket_share.start()
    bucket_share.wait()
    lane256 = iota((TOK, 256), 1)
    count_mat = one_hot((lane256 >= TOK) | (iota((TOK, 256), 0) < lane256))
    ids = iota((8, CHIPS, TOK), 1)
    ids_f = ids.astype(F32)

    def rank_first(i, running):
        hot = jnp.where(b_recv[pl.ds(8 * i, 8)] == ids, 1.0, 0.0)
        counts = dot(hot.astype(BF16).reshape(512, TOK), count_mat)
        for a in range(8):
            block = counts[a * CHIPS:(a + 1) * CHIPS]
            first_rank[8 * i + a] = jnp.sum(hot[a] * (block[:, :TOK] + running), axis=0, keepdims=True)
            running = running + block[:, TOK:]
        return running

    totals = lax.fori_loop(0, 8, rank_first, jnp.zeros((CHIPS, TOK), F32))
    high = jnp.floor(totals * (1.0 / 64))
    low = totals - 64.0 * high
    below = one_hot(iota((CHIPS, CHIPS), 1) < iota((CHIPS, CHIPS), 0))
    offsets = 64.0 * dot(below, high.astype(BF16)) + dot(below, low.astype(BF16))
    shift = (core * HALF).astype(F32)
    within = iota((8, 1, TOK), 0)
    lane_id = iota((CHIPS, TOK), 1)

    def rank_second(i, chunk_counts):
        hot = jnp.where(b_recv[pl.ds(8 * i, 8)] == ids, 1.0, 0.0)
        rank = first_rank[pl.ds(8 * i, 8)] + jnp.sum(hot * offsets[None], axis=1, keepdims=True)
        chunk = jnp.floor(rank * (1.0 / CHUNK)) - shift
        chunk = jnp.where(chunk < 0.0, chunk + float(CHIPS), chunk)
        hot = jnp.where(chunk == ids_f, 1.0, 0.0)
        counts = dot(hot.astype(BF16).reshape(512, TOK), count_mat)
        slot = jnp.sum(hot * counts[:, :TOK].reshape(8, CHIPS, TOK), axis=1, keepdims=True)
        two = jnp.floor(chunk * 0.5)
        code_pair[pl.ds(8 * i, 8)] = chunk * 8.0 + slot + ((within % 2) * SLOTS).astype(F32)
        code_quad[pl.ds(8 * i, 8)] = two * 16.0 + slot + ((within % 4) * SLOTS).astype(F32)
        parity[pl.ds(8 * i, 8)] = chunk - 2.0 * two
        for a in range(8):
            spot = (8 * i + a + core * HALF) % CHIPS
            chunk_counts = chunk_counts + jnp.where(lane_id == spot, counts[a * CHIPS:(a + 1) * CHIPS, TOK:], 0.0)
        return chunk_counts

    chunk_counts = lax.fori_loop(0, 8, rank_second, jnp.zeros((CHIPS, TOK), F32)).astype(BF16)
    source = iota((TOK, 256), 1) // SLOTS
    sources = iota((TOK, 256), 0)
    base = dot(chunk_counts, one_hot(sources < source))
    filled = dot(chunk_counts, one_hot(sources == source))
    slot_no = (iota((CHIPS, 256), 1) % SLOTS).astype(F32)
    slot_rank[...] = jnp.where(slot_no < filled, base + slot_no, -1.0)

    rank_ids = iota((CHUNK, 256), 0).astype(F32)
    ids_quad = iota((512, 512), 0).astype(F32)

    def make_picks(i, _):
        for a in range(11):
            u = 11 * i + a
            picks[u] = one_hot(slot_rank[pl.ds((u + CHIPS - 1) % CHIPS, 1), :] == rank_ids)
        return 0

    lax.fori_loop(0, (HALF + 1) // 11, make_picks, 0)

    def make_hots(quad, _):
        token = core * HALF + quad * 4
        codes = jnp.concatenate([code_quad[token + a] for a in range(4)], axis=1)
        token_hot[quad] = one_hot(codes == ids_quad)
        return 0

    lax.fori_loop(0, 8, make_hots, 0)

    owner_group = chip % 4
    ids512 = iota((512, 256), 0).astype(F32)

    def share(quad):
        return remote(slots_out.at[:, quad], slots.at[:, 8 + quad], s_send_sem.at[quad], s_recv_sem.at[quad], other, chip)

    def to_slots(i, _):
        octet = (owner_group + 4 - i) % 4
        for n in range(8):
            row = r_recv.at[octet * 8 + n]
            pltpu.make_async_copy(row, row, r_recv_sem.at[octet * 8 + n]).wait()
        tiles = []
        for a in range(4):
            spot = octet * 8 + a * 2
            token = core * HALF + spot
            codes = jnp.concatenate([code_pair[token], code_pair[token + 1]], axis=1)
            rows = jnp.concatenate([r_recv[spot], r_recv[spot + 1]], axis=1)
            tiles.append(dot(one_hot(codes == ids512), rows, NT).reshape(CHIPS, 8, TOK))
        for r in range(2):
            quad = 2 * octet + r
            tile = jnp.concatenate(tiles[2 * r:2 * r + 2], axis=1).astype(BF16)
            slots_out[1:1 + HALF, quad] = tile[HALF:]
            slots_out[0, quad] = tile[HALF - 1]
            share(quad).start()
            slots[1:1 + HALF, quad] = tile[:HALF]
            slots[0, quad] = tile[CHIPS - 1]
        return 0

    lax.fori_loop(0, 4, to_slots, 0)

    def gather_own(i, _):
        spots = [11 * i + a for a in range(11)]
        for u in spots:
            found_own[u] = dot(picks[u, :, :CHUNK], slots[u, :8].reshape(CHUNK, TOK)).astype(BF16)
        return 0

    lax.fori_loop(0, (HALF + 1) // 11, gather_own, 0)

    def share_wait(quad, _):
        share(quad).wait()
        return 0

    lax.fori_loop(0, 8, share_wait, 0)

    pick_vals = one_hot(iota((DIM, TOK), 0) + DIM == iota((DIM, TOK), 1))

    def gather_chunks(i, _):
        spots = [11 * i + a for a in range(11)]
        found = [found_own[u].astype(F32) + dot(picks[u, :, CHUNK:], slots[u, 8:].reshape(CHUNK, TOK)) for u in spots]
        for u, rows in zip(spots, found):
            q_wide = rows[:, :DIM]
            inverse = lax.rsqrt(jnp.sum(q_wide * q_wide, axis=1, keepdims=True))
            keys[u] = (q_wide * inverse).astype(BF16)
            narrow = rows.astype(BF16)
            qrows[u] = narrow[:, :DIM]
            vals[u] = dot(pick_vals, narrow, NT).astype(BF16)
        return 0

    lax.fori_loop(0, (HALF + 1) // 11, gather_chunks, 0)
    diagonal = iota((CHUNK, CHUNK), 0) == iota((CHUNK, CHUNK), 1)

    def back_share(n):
        return remote(back_out.at[:, pl.ds(4 * n, 4)], back.at[:, pl.ds(16 + 4 * n, 4)],
                      k_send_sem.at[n], k_recv_sem.at[n], other, chip)

    def softmax(both):
        before, now = both[:CHUNK], jnp.where(diagonal, MASKED, both[CHUNK:])
        top = jnp.maximum(jnp.max(before, axis=0, keepdims=True), jnp.max(now, axis=0, keepdims=True))
        before = jnp.exp2((before - top) * EXP_SCALE)
        now = jnp.exp2((now - top) * EXP_SCALE)
        total = jnp.sum(before, axis=0, keepdims=True) + jnp.sum(now, axis=0, keepdims=True)
        inverse = 1.0 / total
        return jnp.concatenate([(before * inverse).astype(BF16), (now * inverse).astype(BF16)], axis=0)

    def attend(n, _):
        spots = [8 * n + a + 1 for a in range(8)]
        scores = [dot(keys[pl.ds(u - 1, 2)].reshape(2 * CHUNK, DIM), qrows[u], NT) for u in spots]
        probs = [softmax(both) for both in scores]
        outs = [dot(jnp.concatenate([vals[u - 1], vals[u]], axis=1), p).astype(BF16) for u, p in zip(spots, probs)]
        spread = [dot(o, picks[u]) for u, o in zip(spots, outs)]
        for m in range(4):
            tile = jnp.concatenate(spread[2 * m:2 * m + 2], axis=0).T.astype(BF16).reshape(16, 16, TOK)
            back[:, 4 * n + m] = tile[:8]
            back_out[:, 4 * n + m] = tile[8:]

        back_share(n).start()
        return 0

    lax.fori_loop(0, HALF // 8, attend, 0)

    def tokens_own(i, _):
        for a in range(2):
            quad = 2 * i + a
            token_own[quad] = dot(back[quad, :16].reshape(256, TOK), token_hot[quad, :256], TN).astype(BF16)
        return 0

    lax.fori_loop(0, 4, tokens_own, 0)

    def back_wait(n, _):
        back_share(n).wait()
        return 0

    lax.fori_loop(0, 4, back_wait, 0)

    my_batch = place // HEADS
    my_pair = my_batch * HEADS + (chip % 4) * 4 + (chip // 4) % 4

    def to_tokens(i, _):
        quads = [((i // 2 + my_batch) % 2) * 4 + (2 * i + m + chip) % 4 for m in range(2)]
        late = [dot(back[quad, 16:].reshape(256, TOK), token_hot[quad, 256:], TN) for quad in quads]
        for quad, part in zip(quads, late):
            token = core * HALF + quad * 4
            odd = jnp.concatenate([parity[token + a] for a in range(4)], axis=1)
            both = part + token_own[quad].astype(F32)
            rows = jnp.where(odd > 0.5, both[DIM:], both[:DIM]).astype(BF16)
            for a in range(4):
                o_send[quad * 4 + a] = rows[:, a * TOK:(a + 1) * TOK]
        for quad in quads:
            for n in range(4):
                a = (n + chip // 4 + chip // 16) % 4
                target = core * HALF + quad * 4 + a

                @pl.when((target == chip) & mine)
                def _():
                    pltpu.make_async_copy(o_send.at[quad * 4 + a], o_recv.at[my_pair], o_recv_sem.at[my_pair]).start()

                @pl.when((target != chip) | jnp.logical_not(mine))
                def _():
                    remote(o_send.at[quad * 4 + a], o_recv.at[my_pair], o_send_sem, o_recv_sem.at[my_pair], half, target).start()
        return 0

    lax.fori_loop(0, 4, to_tokens, 0)
    for load in wo_loads:
        load.wait()

    def part_share(b, n):
        return remote(acc.at[b, other, n], part_recv.at[b, n], p_send_sem.at[b, n], p_recv_sem.at[b, n], other, chip)

    my_quad = place // 4

    def project_out(i, _):
        b = (i // 4 + my_quad // 4) % 2
        group = (my_quad + 4 - i % 4) % 4
        first = b * HEADS + group * 4
        for n in range(4):
            row = o_recv.at[first + n]
            pltpu.make_async_copy(row, row, o_recv_sem.at[first + n]).wait()
        lhs = o_recv[pl.ds(first, 4)].reshape(256, TOK)
        for side in (other, core):
            for n in range(2):
                acc[b, side, n] += dot(lhs, wo_buf[group, :, pl.ds(pl.multiple_of(side * 1024 + n * 512, 512), 512)], TN)
                if side is other:
                    @pl.when(i % 4 == 3)
                    def _():
                        part_share(b, n).start()
        return 0

    lax.fori_loop(0, 8, project_out, 0)

    def finish(i, _):
        b = (i + my_quad // 4) % 2
        for n in range(2):
            part_share(b, n).wait()
            y_ref[b, :, n * 512:(n + 1) * 512] = (acc[b, core, n] + part_recv[b, n]).astype(BF16)
        return 0

    lax.fori_loop(0, 2, finish, 0)

    @pl.when(mine)
    def _():
        pltpu.make_async_copy(b_send.at[0:31], b_send.at[0:31], b_send_sem).wait()
        pltpu.make_async_copy(r_send.at[0:31], r_send.at[0:31], r_send_sem).wait()
        pltpu.make_async_copy(o_send.at[0:31], o_send.at[0:31], o_send_sem).wait()

    @pl.when(jnp.logical_not(mine))
    def _():
        pltpu.make_async_copy(b_send, b_send, b_send_sem).wait()
        pltpu.make_async_copy(r_send, r_send, r_send_sem).wait()
        pltpu.make_async_copy(o_send, o_send, o_send_sem).wait()


def solution(mesh):
    def step(hidden, bucket, w_qk, w_v, w_o):
        x = hidden.reshape(2 * TOK, MODEL)
        wq = jnp.transpose(w_qk, (1, 2, 0)).reshape(HEADS * DIM, MODEL)
        wv = jnp.transpose(w_v, (1, 2, 0)).reshape(HEADS * DIM, MODEL)
        wo = w_o.reshape(4, 256, MODEL)
        any_spec = pl.BlockSpec(memory_space=pl.ANY)
        vmem_spec = pl.BlockSpec(memory_space=pltpu.VMEM)
        dma = pltpu.SemaphoreType.DMA
        return pl.pallas_call(
            kernel,
            out_shape=pltpu.VMEM((2, TOK, MODEL // 2), BF16),
            in_specs=[any_spec, vmem_spec, any_spec, any_spec, any_spec],
            out_specs=vmem_spec,
            scratch_shapes=[
                pltpu.VMEM((2 * TOK, MODEL), BF16),
                pltpu.VMEM((4, 2, 256, MODEL), BF16),
                pltpu.VMEM((4, 256, MODEL), BF16),
                pltpu.VMEM((HALF, 1, TOK), jnp.int32),
                pltpu.VMEM((CHIPS, 1, TOK), jnp.int32),
                pltpu.VMEM((HALF, 2 * DIM, TOK), BF16),
                pltpu.VMEM((HALF, 2 * DIM, TOK), BF16),
                pltpu.VMEM((CHIPS, 1, TOK), F32),
                pltpu.VMEM((CHIPS, 1, TOK), F32),
                pltpu.VMEM((CHIPS, 1, TOK), F32),
                pltpu.VMEM((CHIPS, 1, TOK), F32),
                pltpu.VMEM((CHIPS, 256), F32),
                pltpu.VMEM((HALF + 1, 16, 16, TOK), BF16),
                pltpu.VMEM((HALF + 1, 8, 16, TOK), BF16),
                pltpu.VMEM((HALF + 1, CHUNK, 256), BF16),
                pltpu.VMEM((8, 512, 512), BF16),
                pltpu.VMEM((HALF + 1, CHUNK, TOK), BF16),
                pltpu.VMEM((8, TOK, 512), BF16),
                pltpu.VMEM((HALF + 1, CHUNK, DIM), BF16),
                pltpu.VMEM((HALF + 1, DIM, CHUNK), BF16),
                pltpu.VMEM((HALF + 1, CHUNK, DIM), BF16),
                pltpu.VMEM((8, HALF, 16, TOK), BF16),
                pltpu.VMEM((8, HALF // 2, 16, TOK), BF16),
                pltpu.VMEM((HALF, DIM, TOK), BF16),
                pltpu.VMEM((HALF, DIM, TOK), BF16),
                pltpu.VMEM((2, 2, 2, TOK, 512), F32),
                pltpu.VMEM((2, 2, TOK, 512), F32),
                dma((13,)), dma(()), dma(()), dma((2,)), dma(()), dma((HALF,)), dma((8,)), dma((8,)),
                dma((4,)), dma((4,)), dma(()), dma((HALF,)), dma((2, 2)), dma((2, 2)),
            ],
            compiler_params=pltpu.CompilerParams(collective_id=0, has_side_effects=True, vmem_limit_bytes=56 * 1024 * 1024),
            name="bucket_attention",
        )(x, bucket, wq, wv, wo)

    return jax.shard_map(
        step, mesh=mesh,
        in_specs=(P("dp", "sp", None), P("dp", "tp", "sp"), P(None, "tp", None), P(None, "tp", None), P("tp", None, None)),
        out_specs=P("dp", "sp", "tp"), check_vma=False)
```

```python
import functools

import jax
import jax.numpy as jnp
from jax import lax
from jax.experimental import pallas as pl
from jax.experimental.pallas import tpu as pltpu
from jax.sharding import PartitionSpec as P

CHIPS = 64
HALF = 32
TOK = 128
CHUNK = 128
HEADS = 16
DIM = 64
MODEL = 2048
SLOTS = 4
SPAN = 32
MASKED = -8e5
EXP_SCALE = 0.125 * 1.4426950408889634
F32 = jnp.float32
BF16 = jnp.bfloat16
NT = (((1,), (1,)), ((), ()))
TN = (((0,), (0,)), ((), ()))


def iota(shape, axis):
    return lax.broadcasted_iota(jnp.int32, shape, axis)


def one_hot(mask):
    return jnp.where(mask, 1.0, 0.0).astype(BF16)


def dot(a, b, dims=(((1,), (0,)), ((), ()))):
    return lax.dot_general(a, b, dims, preferred_element_type=F32)


def kernel(x_hbm, bucket_ref, wq_hbm, wv_hbm, wo_hbm, y_ref,
           x_buf, w_buf, wo_buf, b_send, b_recv, r_send, r_recv,
           first_rank, code_pair, code_quad, parity, slot_rank,
           slots, slots_out, picks, token_hot, found_own, token_own, keys, vals, qrows, back, back_out, o_send, o_recv, acc, part_recv,
           load_sem, b_send_sem, b_recv_sem, b_pass_sem, r_send_sem, r_recv_sem, s_send_sem, s_recv_sem,
           k_send_sem, k_recv_sem, o_send_sem, o_recv_sem, p_send_sem, p_recv_sem):
    core = lax.axis_index("tp")
    chip = lax.axis_index("sp")
    other = 1 - core
    half = chip // HALF
    place = chip % HALF
    mine = core == half

    def peer(t, s):
        return {"dp": 0, "tp": t, "sp": s}

    def remote(src, dst, send, recv, t, s):
        return pltpu.make_async_remote_copy(
            src_ref=src, dst_ref=dst, send_sem=send, recv_sem=recv,
            device_id=peer(t, s), device_id_type=pl.DeviceIdType.MESH)

    turn = (chip // 8) % 4
    x_load = pltpu.make_async_copy(x_hbm, x_buf, load_sem.at[0])
    x_load.start()

    def w_loads(step):
        group = (step + turn) % 4
        return (pltpu.make_async_copy(wq_hbm.at[pl.ds(group * 256, 256)], w_buf.at[step, 0], load_sem.at[1 + step]),
                pltpu.make_async_copy(wv_hbm.at[pl.ds(group * 256, 256)], w_buf.at[step, 1], load_sem.at[5 + step]))

    for step in range(4):
        for load in w_loads(step):
            load.start()
    wo_loads = [pltpu.make_async_copy(wo_hbm.at[g], wo_buf.at[g], load_sem.at[9 + g]) for g in range(4)]
    for load in wo_loads:
        load.start()

    barrier = pltpu.get_barrier_semaphore()

    def greet(t, s):
        pl.semaphore_signal(barrier, inc=1, device_id=peer(t, s), device_id_type=pl.DeviceIdType.MESH)

    def greet_chip(i, _):
        spot = (place + i) % HALF
        greet(0, core * HALF + spot)
        greet(1, core * HALF + spot)
        greet(half, other * HALF + spot)
        return 0

    lax.fori_loop(1, HALF, greet_chip, 0)
    greet(half, other * HALF + place)
    greet(1 - half, core * HALF + place)

    @pl.when(jnp.logical_not(mine))
    def _():
        greet(half, core * HALF + place)

    for b in range(2):
        for h in range(HEADS):
            b_send[b * HEADS + h] = bucket_ref[b, h:h + 1, :]

    x_load.wait()

    def project(step):
        for load in w_loads(step):
            load.wait()
        group = (step + turn) % 4
        rows = dot(w_buf[step].reshape(512, MODEL), x_buf[...], NT).astype(BF16)
        for hh in range(4):
            for b in range(2):
                pair = b * HEADS + group * 4 + hh
                r_send[pair, 0:DIM] = rows[hh * DIM:(hh + 1) * DIM, b * TOK:(b + 1) * TOK]
                r_send[pair, DIM:2 * DIM] = rows[256 + hh * DIM:256 + (hh + 1) * DIM, b * TOK:(b + 1) * TOK]

    def send_rows(step):
        group = (step + turn) % 4

        def body(i, _):
            spot = (i + chip // 4 + chip // 16) % 8
            pair = (spot // 4) * HEADS + group * 4 + spot % 4
            target = core * HALF + (spot // 4) * HEADS + (spot % 4) * 4 + group

            @pl.when((target == chip) & mine)
            def _():
                pltpu.make_async_copy(r_send.at[pair], r_recv.at[place], r_recv_sem.at[place]).start()

            @pl.when((target != chip) | jnp.logical_not(mine))
            def _():
                remote(r_send.at[pair], r_recv.at[place], r_send_sem, r_recv_sem.at[place], half, target).start()
            return 0

        lax.fori_loop(0, 8, body, 0)

    def send_buckets(i, _):
        spot = (i + place) % HALF
        pair = (spot // HEADS) * HEADS + (spot % 4) * 4 + (spot // 4) % 4
        target = core * HALF + spot

        @pl.when((i == 0) & mine)
        def _():
            pltpu.make_async_copy(b_send.at[pair], b_recv.at[chip], b_recv_sem).start()

        @pl.when((i > 0) | jnp.logical_not(mine))
        def _():
            remote(b_send.at[pair], b_recv.at[chip], b_send_sem, b_recv_sem, half, target).start()
        return 0

    project(0)
    acc[...] = jnp.zeros_like(acc)
    @pl.when(mine)
    def _():
        pl.semaphore_wait(barrier, 95)

    @pl.when(jnp.logical_not(mine))
    def _():
        pl.semaphore_wait(barrier, 96)

    lax.fori_loop(0, HALF, send_buckets, 0)
    send_rows(0)

    def project_more(step, _):
        project(step)
        send_rows(step)
        return 0

    lax.fori_loop(1, 4, project_more, 0)

    own_rows = b_recv.at[pl.ds(core * HALF, HALF)]
    pltpu.make_async_copy(own_rows, own_rows, b_recv_sem).wait()
    bucket_share = remote(own_rows, own_rows, b_pass_sem.at[0], b_pass_sem.at[1], other, chip)
    bucket_share.start()
    bucket_share.wait()
    lane256 = iota((TOK, 256), 1)
    count_mat = one_hot((lane256 >= TOK) | (iota((TOK, 256), 0) < lane256))
    ids = iota((SPAN, CHIPS, TOK), 1)
    ids_f = ids.astype(F32)

    def rank_first(i, running):
        hot = jnp.where(b_recv[pl.ds(SPAN * i, SPAN)] == ids, 1.0, 0.0)
        counts = dot(hot.astype(BF16).reshape(SPAN * CHIPS, TOK), count_mat)
        for a in range(SPAN):
            block = counts[a * CHIPS:(a + 1) * CHIPS]
            first_rank[SPAN * i + a] = jnp.sum(hot[a] * (block[:, :TOK] + running), axis=0, keepdims=True)
            running = running + block[:, TOK:]
        return running

    totals = lax.fori_loop(0, CHIPS // SPAN, rank_first, jnp.zeros((CHIPS, TOK), F32))
    high = jnp.floor(totals * (1.0 / 64))
    low = totals - 64.0 * high
    below = one_hot(iota((CHIPS, CHIPS), 1) < iota((CHIPS, CHIPS), 0))
    offsets = 64.0 * dot(below, high.astype(BF16)) + dot(below, low.astype(BF16))
    shift = (core * HALF).astype(F32)
    within = iota((SPAN, 1, TOK), 0)
    lane_id = iota((CHIPS, TOK), 1)

    def rank_second(i, chunk_counts):
        hot = jnp.where(b_recv[pl.ds(SPAN * i, SPAN)] == ids, 1.0, 0.0)
        rank = first_rank[pl.ds(SPAN * i, SPAN)] + jnp.sum(hot * offsets[None], axis=1, keepdims=True)
        chunk = jnp.floor(rank * (1.0 / CHUNK)) - shift
        chunk = jnp.where(chunk < 0.0, chunk + float(CHIPS), chunk)
        hot = jnp.where(chunk == ids_f, 1.0, 0.0)
        counts = dot(hot.astype(BF16).reshape(SPAN * CHIPS, TOK), count_mat)
        slot = jnp.sum(hot * counts[:, :TOK].reshape(SPAN, CHIPS, TOK), axis=1, keepdims=True)
        two = jnp.floor(chunk * 0.5)
        code_pair[pl.ds(SPAN * i, SPAN)] = chunk * 8.0 + slot + ((within % 2) * SLOTS).astype(F32)
        code_quad[pl.ds(SPAN * i, SPAN)] = two * 16.0 + slot + ((within % 4) * SLOTS).astype(F32)
        parity[pl.ds(SPAN * i, SPAN)] = chunk - 2.0 * two
        for a in range(SPAN):
            spot = (SPAN * i + a + core * HALF) % CHIPS
            chunk_counts = chunk_counts + jnp.where(lane_id == spot, counts[a * CHIPS:(a + 1) * CHIPS, TOK:], 0.0)
        return chunk_counts

    chunk_counts = lax.fori_loop(0, CHIPS // SPAN, rank_second, jnp.zeros((CHIPS, TOK), F32)).astype(BF16)
    source = iota((TOK, 256), 1) // SLOTS
    sources = iota((TOK, 256), 0)
    base = dot(chunk_counts, one_hot(sources < source))
    filled = dot(chunk_counts, one_hot(sources == source))
    slot_no = (iota((CHIPS, 256), 1) % SLOTS).astype(F32)
    slot_rank[...] = jnp.where(slot_no < filled, base + slot_no, -1.0)

    rank_ids = iota((CHUNK, 256), 0).astype(F32)
    ids_quad = iota((512, 512), 0).astype(F32)

    def make_picks(i, _):
        for a in range(11):
            u = 11 * i + a
            picks[u] = one_hot(slot_rank[pl.ds((u + CHIPS - 1) % CHIPS, 1), :] == rank_ids)
        return 0

    lax.fori_loop(0, (HALF + 1) // 11, make_picks, 0)

    def make_hots(quad, _):
        token = core * HALF + quad * 4
        codes = jnp.concatenate([code_quad[token + a] for a in range(4)], axis=1)
        token_hot[quad] = one_hot(codes == ids_quad)
        return 0

    lax.fori_loop(0, 8, make_hots, 0)

    owner_group = chip % 4
    ids512 = iota((512, 256), 0).astype(F32)

    def share(quad):
        return remote(slots_out.at[:, quad], slots.at[:, 8 + quad], s_send_sem.at[quad], s_recv_sem.at[quad], other, chip)

    def to_slots(i, _):
        octet = (owner_group + 4 - i) % 4
        for n in range(8):
            row = r_recv.at[octet * 8 + n]
            pltpu.make_async_copy(row, row, r_recv_sem.at[octet * 8 + n]).wait()
        tiles = []
        for a in range(4):
            spot = octet * 8 + a * 2
            token = core * HALF + spot
            codes = jnp.concatenate([code_pair[token], code_pair[token + 1]], axis=1)
            rows = jnp.concatenate([r_recv[spot], r_recv[spot + 1]], axis=1)
            tiles.append(dot(one_hot(codes == ids512), rows, NT).reshape(CHIPS, 8, TOK))
        for r in range(2):
            quad = 2 * octet + r
            tile = jnp.concatenate(tiles[2 * r:2 * r + 2], axis=1).astype(BF16)
            slots_out[1:1 + HALF, quad] = tile[HALF:]
            slots_out[0, quad] = tile[HALF - 1]
            share(quad).start()
            slots[1:1 + HALF, quad] = tile[:HALF]
            slots[0, quad] = tile[CHIPS - 1]
        return 0

    lax.fori_loop(0, 4, to_slots, 0)

    def gather_own(i, _):
        spots = [33 * i + a for a in range(33)]
        for u in spots:
            found_own[u] = dot(picks[u, :, :CHUNK], slots[u, :8].reshape(CHUNK, TOK)).astype(BF16)
        return 0

    lax.fori_loop(0, (HALF + 1) // 33, gather_own, 0)

    def share_wait(quad, _):
        share(quad).wait()
        return 0

    lax.fori_loop(0, 8, share_wait, 0)

    pick_vals = one_hot(iota((DIM, TOK), 0) + DIM == iota((DIM, TOK), 1))

    def gather_chunks(i, _):
        spots = [33 * i + a for a in range(33)]
        found = [found_own[u].astype(F32) + dot(picks[u, :, CHUNK:], slots[u, 8:].reshape(CHUNK, TOK)) for u in spots]
        for u, rows in zip(spots, found):
            q_wide = rows[:, :DIM]
            inverse = lax.rsqrt(jnp.sum(q_wide * q_wide, axis=1, keepdims=True))
            keys[u] = (q_wide * inverse).astype(BF16)
            narrow = rows.astype(BF16)
            qrows[u] = narrow[:, :DIM]
            vals[u] = dot(pick_vals, narrow, NT).astype(BF16)
        return 0

    lax.fori_loop(0, (HALF + 1) // 33, gather_chunks, 0)
    diagonal = iota((CHUNK, CHUNK), 0) == iota((CHUNK, CHUNK), 1)

    def back_share(n):
        return remote(back_out.at[:, pl.ds(4 * n, 4)], back.at[:, pl.ds(16 + 4 * n, 4)],
                      k_send_sem.at[n], k_recv_sem.at[n], other, chip)

    def softmax(both):
        before, now = both[:CHUNK], jnp.where(diagonal, MASKED, both[CHUNK:])
        top = jnp.maximum(jnp.max(before, axis=0, keepdims=True), jnp.max(now, axis=0, keepdims=True))
        before = jnp.exp2((before - top) * EXP_SCALE)
        now = jnp.exp2((now - top) * EXP_SCALE)
        total = jnp.sum(before, axis=0, keepdims=True) + jnp.sum(now, axis=0, keepdims=True)
        inverse = 1.0 / total
        return jnp.concatenate([(before * inverse).astype(BF16), (now * inverse).astype(BF16)], axis=0)

    def attend(n, _):
        spots = [32 * n + a + 1 for a in range(32)]
        scores = [dot(keys[pl.ds(u - 1, 2)].reshape(2 * CHUNK, DIM), qrows[u], NT) for u in spots]
        probs = [softmax(both) for both in scores]
        outs = [dot(jnp.concatenate([vals[u - 1], vals[u]], axis=1), p).astype(BF16) for u, p in zip(spots, probs)]
        spread = [dot(o, picks[u]) for u, o in zip(spots, outs)]
        for m in range(16):
            tile = jnp.concatenate(spread[2 * m:2 * m + 2], axis=0).T.astype(BF16).reshape(16, 16, TOK)
            back[:, 16 * n + m] = tile[:8]
            back_out[:, 16 * n + m] = tile[8:]

        for part in range(4):
            back_share(part).start()
        return 0

    lax.fori_loop(0, HALF // 32, attend, 0)

    def tokens_own(i, _):
        for a in range(4):
            quad = 4 * i + a
            token_own[quad] = dot(back[quad, :16].reshape(256, TOK), token_hot[quad, :256], TN).astype(BF16)
        return 0

    lax.fori_loop(0, 2, tokens_own, 0)

    def back_wait(n, _):
        back_share(n).wait()
        return 0

    lax.fori_loop(0, 4, back_wait, 0)

    my_batch = place // HEADS
    my_pair = my_batch * HEADS + (chip % 4) * 4 + (chip // 4) % 4

    def to_tokens(i, _):
        quads = [((i // 2 + my_batch) % 2) * 4 + (2 * i + m + chip) % 4 for m in range(2)]
        late = [dot(back[quad, 16:].reshape(256, TOK), token_hot[quad, 256:], TN) for quad in quads]
        for quad, part in zip(quads, late):
            token = core * HALF + quad * 4
            odd = jnp.concatenate([parity[token + a] for a in range(4)], axis=1)
            both = part + token_own[quad].astype(F32)
            rows = jnp.where(odd > 0.5, both[DIM:], both[:DIM]).astype(BF16)
            for a in range(4):
                o_send[quad * 4 + a] = rows[:, a * TOK:(a + 1) * TOK]
        for quad in quads:
            for n in range(4):
                a = (n + chip + chip // 4 + chip // 16) % 4
                target = core * HALF + quad * 4 + a

                @pl.when((target == chip) & mine)
                def _():
                    pltpu.make_async_copy(o_send.at[quad * 4 + a], o_recv.at[my_pair], o_recv_sem.at[my_pair]).start()

                @pl.when((target != chip) | jnp.logical_not(mine))
                def _():
                    remote(o_send.at[quad * 4 + a], o_recv.at[my_pair], o_send_sem, o_recv_sem.at[my_pair], half, target).start()
        return 0

    lax.fori_loop(0, 4, to_tokens, 0)
    for load in wo_loads:
        load.wait()

    def part_share(b, n):
        return remote(acc.at[b, other, n], part_recv.at[b, n], p_send_sem.at[b, n], p_recv_sem.at[b, n], other, chip)

    my_quad = place // 4

    def project_out(i, _):
        b = (i // 4 + my_quad // 4) % 2
        group = (my_quad + 4 - i % 4) % 4
        first = b * HEADS + group * 4
        for n in range(4):
            row = o_recv.at[first + n]
            pltpu.make_async_copy(row, row, o_recv_sem.at[first + n]).wait()
        lhs = o_recv[pl.ds(first, 4)].reshape(256, TOK)
        for side in (other, core):
            for n in range(2):
                acc[b, side, n] += dot(lhs, wo_buf[group, :, pl.ds(pl.multiple_of(side * 1024 + n * 512, 512), 512)], TN)
                if side is other:
                    @pl.when(i % 4 == 3)
                    def _():
                        part_share(b, n).start()
        return 0

    lax.fori_loop(0, 8, project_out, 0)

    def finish(i, _):
        b = (i + my_quad // 4) % 2
        for n in range(2):
            part_share(b, n).wait()
            y_ref[b, :, n * 512:(n + 1) * 512] = (acc[b, core, n] + part_recv[b, n]).astype(BF16)
        return 0

    lax.fori_loop(0, 2, finish, 0)

    @pl.when(mine)
    def _():
        pltpu.make_async_copy(b_send.at[0:31], b_send.at[0:31], b_send_sem).wait()
        pltpu.make_async_copy(r_send.at[0:31], r_send.at[0:31], r_send_sem).wait()
        pltpu.make_async_copy(o_send.at[0:31], o_send.at[0:31], o_send_sem).wait()

    @pl.when(jnp.logical_not(mine))
    def _():
        pltpu.make_async_copy(b_send, b_send, b_send_sem).wait()
        pltpu.make_async_copy(r_send, r_send, r_send_sem).wait()
        pltpu.make_async_copy(o_send, o_send, o_send_sem).wait()


def solution(mesh):
    def step(hidden, bucket, w_qk, w_v, w_o):
        x = hidden.reshape(2 * TOK, MODEL)
        wq = jnp.transpose(w_qk, (1, 2, 0)).reshape(HEADS * DIM, MODEL)
        wv = jnp.transpose(w_v, (1, 2, 0)).reshape(HEADS * DIM, MODEL)
        wo = w_o.reshape(4, 256, MODEL)
        any_spec = pl.BlockSpec(memory_space=pl.ANY)
        vmem_spec = pl.BlockSpec(memory_space=pltpu.VMEM)
        dma = pltpu.SemaphoreType.DMA
        return pl.pallas_call(
            kernel,
            out_shape=pltpu.VMEM((2, TOK, MODEL // 2), BF16),
            in_specs=[any_spec, vmem_spec, any_spec, any_spec, any_spec],
            out_specs=vmem_spec,
            scratch_shapes=[
                pltpu.VMEM((2 * TOK, MODEL), BF16),
                pltpu.VMEM((4, 2, 256, MODEL), BF16),
                pltpu.VMEM((4, 256, MODEL), BF16),
                pltpu.VMEM((HALF, 1, TOK), jnp.int32),
                pltpu.VMEM((CHIPS, 1, TOK), jnp.int32),
                pltpu.VMEM((HALF, 2 * DIM, TOK), BF16),
                pltpu.VMEM((HALF, 2 * DIM, TOK), BF16),
                pltpu.VMEM((CHIPS, 1, TOK), F32),
                pltpu.VMEM((CHIPS, 1, TOK), F32),
                pltpu.VMEM((CHIPS, 1, TOK), F32),
                pltpu.VMEM((CHIPS, 1, TOK), F32),
                pltpu.VMEM((CHIPS, 256), F32),
                pltpu.VMEM((HALF + 1, 16, 16, TOK), BF16),
                pltpu.VMEM((HALF + 1, 8, 16, TOK), BF16),
                pltpu.VMEM((HALF + 1, CHUNK, 256), BF16),
                pltpu.VMEM((8, 512, 512), BF16),
                pltpu.VMEM((HALF + 1, CHUNK, TOK), BF16),
                pltpu.VMEM((8, TOK, 512), BF16),
                pltpu.VMEM((HALF + 1, CHUNK, DIM), BF16),
                pltpu.VMEM((HALF + 1, DIM, CHUNK), BF16),
                pltpu.VMEM((HALF + 1, CHUNK, DIM), BF16),
                pltpu.VMEM((8, HALF, 16, TOK), BF16),
                pltpu.VMEM((8, HALF // 2, 16, TOK), BF16),
                pltpu.VMEM((HALF, DIM, TOK), BF16),
                pltpu.VMEM((HALF, DIM, TOK), BF16),
                pltpu.VMEM((2, 2, 2, TOK, 512), F32),
                pltpu.VMEM((2, 2, TOK, 512), F32),
                dma((13,)), dma(()), dma(()), dma((2,)), dma(()), dma((HALF,)), dma((8,)), dma((8,)),
                dma((4,)), dma((4,)), dma(()), dma((HALF,)), dma((2, 2)), dma((2, 2)),
            ],
            compiler_params=pltpu.CompilerParams(collective_id=0, has_side_effects=True, vmem_limit_bytes=56 * 1024 * 1024),
            name="bucket_attention",
        )(x, bucket, wq, wv, wo)

    return jax.shard_map(
        step, mesh=mesh,
        in_specs=(P("dp", "sp", None), P("dp", "tp", "sp"), P(None, "tp", None), P(None, "tp", None), P("tp", None, None)),
        out_specs=P("dp", "sp", "tp"), check_vma=False)
```

```python
import functools

import jax
import jax.numpy as jnp
from jax import lax
from jax.experimental import pallas as pl
from jax.experimental.pallas import tpu as pltpu
from jax.sharding import PartitionSpec as P

CHIPS = 64
HALF = 32
TOK = 128
CHUNK = 128
HEADS = 16
DIM = 64
MODEL = 2048
SLOTS = 4
SPAN = 32
MASKED = -8e5
EXP_SCALE = 0.125 * 1.4426950408889634
F32 = jnp.float32
BF16 = jnp.bfloat16
NT = (((1,), (1,)), ((), ()))
TN = (((0,), (0,)), ((), ()))


def iota(shape, axis):
    return lax.broadcasted_iota(jnp.int32, shape, axis)


def one_hot(mask):
    return jnp.where(mask, 1.0, 0.0).astype(BF16)


def dot(a, b, dims=(((1,), (0,)), ((), ()))):
    return lax.dot_general(a, b, dims, preferred_element_type=F32)


def kernel(x_hbm, bucket_ref, wq_hbm, wv_hbm, wo_hbm, y_ref,
           x_buf, w_buf, wo_buf, b_send, b_recv, r_send, r_recv,
           first_rank, code_pair, code_quad, parity, slot_rank,
           slots, slots_out, picks, token_hot, found_own, token_own, keys, vals, qrows, back, back_out, o_send, o_recv, o_far, wo_far, acc,
           load_sem, b_send_sem, b_recv_sem, b_pass_sem, r_send_sem, r_recv_sem, s_send_sem, s_recv_sem,
           k_send_sem, k_recv_sem, o_send_sem, o_recv_sem, p_send_sem, p_recv_sem, w_pass_sem):
    core = lax.axis_index("tp")
    chip = lax.axis_index("sp")
    other = 1 - core
    half = chip // HALF
    place = chip % HALF
    mine = core == half

    def peer(t, s):
        return {"dp": 0, "tp": t, "sp": s}

    def remote(src, dst, send, recv, t, s):
        return pltpu.make_async_remote_copy(
            src_ref=src, dst_ref=dst, send_sem=send, recv_sem=recv,
            device_id=peer(t, s), device_id_type=pl.DeviceIdType.MESH)

    turn = (chip // 8) % 4
    x_load = pltpu.make_async_copy(x_hbm, x_buf, load_sem.at[0])
    x_load.start()

    def w_loads(step):
        group = (step + turn) % 4
        return (pltpu.make_async_copy(wq_hbm.at[pl.ds(group * 256, 256)], w_buf.at[step, 0], load_sem.at[1 + step]),
                pltpu.make_async_copy(wv_hbm.at[pl.ds(group * 256, 256)], w_buf.at[step, 1], load_sem.at[5 + step]))

    for step in range(4):
        for load in w_loads(step):
            load.start()
    wo_loads = [pltpu.make_async_copy(wo_hbm.at[g], wo_buf.at[g], load_sem.at[9 + g]) for g in range(4)]
    for load in wo_loads:
        load.start()

    barrier = pltpu.get_barrier_semaphore()

    def greet(t, s):
        pl.semaphore_signal(barrier, inc=1, device_id=peer(t, s), device_id_type=pl.DeviceIdType.MESH)

    def greet_chip(i, _):
        spot = (place + i) % HALF
        greet(0, core * HALF + spot)
        greet(1, core * HALF + spot)
        greet(half, other * HALF + spot)
        return 0

    lax.fori_loop(1, HALF, greet_chip, 0)
    greet(half, other * HALF + place)
    greet(1 - half, core * HALF + place)

    @pl.when(jnp.logical_not(mine))
    def _():
        greet(half, core * HALF + place)

    for b in range(2):
        for h in range(HEADS):
            b_send[b * HEADS + h] = bucket_ref[b, h:h + 1, :]

    x_load.wait()

    def project(step):
        for load in w_loads(step):
            load.wait()
        group = (step + turn) % 4
        rows = dot(w_buf[step].reshape(512, MODEL), x_buf[...], NT).astype(BF16)
        for hh in range(4):
            for b in range(2):
                pair = b * HEADS + group * 4 + hh
                r_send[pair, 0:DIM] = rows[hh * DIM:(hh + 1) * DIM, b * TOK:(b + 1) * TOK]
                r_send[pair, DIM:2 * DIM] = rows[256 + hh * DIM:256 + (hh + 1) * DIM, b * TOK:(b + 1) * TOK]

    def send_rows(step):
        group = (step + turn) % 4

        def body(i, _):
            spot = (chip // 4 + chip // 16 + 8 - i) % 8
            pair = (spot // 4) * HEADS + group * 4 + spot % 4
            target = core * HALF + (spot // 4) * HEADS + (spot % 4) * 4 + group

            @pl.when((target == chip) & mine)
            def _():
                pltpu.make_async_copy(r_send.at[pair], r_recv.at[place], r_recv_sem.at[place]).start()

            @pl.when((target != chip) | jnp.logical_not(mine))
            def _():
                remote(r_send.at[pair], r_recv.at[place], r_send_sem, r_recv_sem.at[place], half, target).start()
            return 0

        lax.fori_loop(0, 8, body, 0)

    def send_buckets(i, _):
        spot = (i + place) % HALF
        pair = (spot // HEADS) * HEADS + (spot % 4) * 4 + (spot // 4) % 4
        target = core * HALF + spot

        @pl.when((i == 0) & mine)
        def _():
            pltpu.make_async_copy(b_send.at[pair], b_recv.at[chip], b_recv_sem).start()

        @pl.when((i > 0) | jnp.logical_not(mine))
        def _():
            remote(b_send.at[pair], b_recv.at[chip], b_send_sem, b_recv_sem, half, target).start()
        return 0

    project(0)
    acc[...] = jnp.zeros_like(acc)
    @pl.when(mine)
    def _():
        pl.semaphore_wait(barrier, 95)

    @pl.when(jnp.logical_not(mine))
    def _():
        pl.semaphore_wait(barrier, 96)

    lax.fori_loop(0, HALF, send_buckets, 0)
    send_rows(0)

    def project_more(step, _):
        project(step)
        send_rows(step)
        return 0

    lax.fori_loop(1, 4, project_more, 0)

    for load in wo_loads:
        load.wait()
    my_columns = pl.ds(pl.multiple_of(core * 1024, 1024), 1024)
    wo_share = remote(wo_buf.at[:, :, pl.ds(pl.multiple_of(other * 1024, 1024), 1024)], wo_far,
                      w_pass_sem.at[0], w_pass_sem.at[1], other, chip)
    wo_share.start()

    own_rows = b_recv.at[pl.ds(core * HALF, HALF)]
    pltpu.make_async_copy(own_rows, own_rows, b_recv_sem).wait()
    bucket_share = remote(own_rows, own_rows, b_pass_sem.at[0], b_pass_sem.at[1], other, chip)
    bucket_share.start()
    bucket_share.wait()
    lane256 = iota((TOK, 256), 1)
    count_mat = one_hot((lane256 >= TOK) | (iota((TOK, 256), 0) < lane256))
    ids = iota((SPAN, CHIPS, TOK), 1)
    ids_f = ids.astype(F32)

    def rank_first(i, running):
        hot = jnp.where(b_recv[pl.ds(SPAN * i, SPAN)] == ids, 1.0, 0.0)
        counts = dot(hot.astype(BF16).reshape(SPAN * CHIPS, TOK), count_mat)
        for a in range(SPAN):
            block = counts[a * CHIPS:(a + 1) * CHIPS]
            first_rank[SPAN * i + a] = jnp.sum(hot[a] * (block[:, :TOK] + running), axis=0, keepdims=True)
            running = running + block[:, TOK:]
        return running

    totals = lax.fori_loop(0, CHIPS // SPAN, rank_first, jnp.zeros((CHIPS, TOK), F32))
    high = jnp.floor(totals * (1.0 / 64))
    low = totals - 64.0 * high
    below = one_hot(iota((CHIPS, CHIPS), 1) < iota((CHIPS, CHIPS), 0))
    offsets = 64.0 * dot(below, high.astype(BF16)) + dot(below, low.astype(BF16))
    shift = (core * HALF).astype(F32)
    within = iota((SPAN, 1, TOK), 0)
    lane_id = iota((CHIPS, TOK), 1)

    def rank_second(i, chunk_counts):
        hot = jnp.where(b_recv[pl.ds(SPAN * i, SPAN)] == ids, 1.0, 0.0)
        rank = first_rank[pl.ds(SPAN * i, SPAN)] + jnp.sum(hot * offsets[None], axis=1, keepdims=True)
        chunk = jnp.floor(rank * (1.0 / CHUNK)) - shift
        chunk = jnp.where(chunk < 0.0, chunk + float(CHIPS), chunk)
        hot = jnp.where(chunk == ids_f, 1.0, 0.0)
        counts = dot(hot.astype(BF16).reshape(SPAN * CHIPS, TOK), count_mat)
        slot = jnp.sum(hot * counts[:, :TOK].reshape(SPAN, CHIPS, TOK), axis=1, keepdims=True)
        two = jnp.floor(chunk * 0.5)
        code_pair[pl.ds(SPAN * i, SPAN)] = chunk * 8.0 + slot + ((within % 2) * SLOTS).astype(F32)
        code_quad[pl.ds(SPAN * i, SPAN)] = two * 16.0 + slot + ((within % 4) * SLOTS).astype(F32)
        parity[pl.ds(SPAN * i, SPAN)] = chunk - 2.0 * two
        for a in range(SPAN):
            spot = (SPAN * i + a + core * HALF) % CHIPS
            chunk_counts = chunk_counts + jnp.where(lane_id == spot, counts[a * CHIPS:(a + 1) * CHIPS, TOK:], 0.0)
        return chunk_counts

    chunk_counts = lax.fori_loop(0, CHIPS // SPAN, rank_second, jnp.zeros((CHIPS, TOK), F32)).astype(BF16)
    source = iota((TOK, 256), 1) // SLOTS
    sources = iota((TOK, 256), 0)
    base = dot(chunk_counts, one_hot(sources < source))
    filled = dot(chunk_counts, one_hot(sources == source))
    slot_no = (iota((CHIPS, 256), 1) % SLOTS).astype(F32)
    slot_rank[...] = jnp.where(slot_no < filled, base + slot_no, -1.0)

    rank_ids = iota((CHUNK, 256), 0).astype(F32)
    ids_quad = iota((512, 512), 0).astype(F32)

    def make_picks(i, _):
        for a in range(11):
            u = 11 * i + a
            picks[u] = one_hot(slot_rank[pl.ds((u + CHIPS - 1) % CHIPS, 1), :] == rank_ids)
        return 0

    lax.fori_loop(0, (HALF + 1) // 11, make_picks, 0)

    def make_hots(quad, _):
        token = core * HALF + quad * 4
        codes = jnp.concatenate([code_quad[token + a] for a in range(4)], axis=1)
        token_hot[quad] = one_hot(codes == ids_quad)
        return 0

    lax.fori_loop(0, 8, make_hots, 0)

    owner_group = chip % 4
    ids512 = iota((512, 256), 0).astype(F32)

    def share(quad):
        return remote(slots_out.at[:, quad], slots.at[:, 8 + quad], s_send_sem.at[quad], s_recv_sem.at[quad], other, chip)

    def to_slots(i, _):
        octet = (owner_group + 4 - i) % 4
        for n in range(8):
            row = r_recv.at[octet * 8 + n]
            pltpu.make_async_copy(row, row, r_recv_sem.at[octet * 8 + n]).wait()
        tiles = []
        for a in range(4):
            spot = octet * 8 + a * 2
            token = core * HALF + spot
            codes = jnp.concatenate([code_pair[token], code_pair[token + 1]], axis=1)
            rows = jnp.concatenate([r_recv[spot], r_recv[spot + 1]], axis=1)
            tiles.append(dot(one_hot(codes == ids512), rows, NT).reshape(CHIPS, 8, TOK))
        for r in range(2):
            quad = 2 * octet + r
            tile = jnp.concatenate(tiles[2 * r:2 * r + 2], axis=1).astype(BF16)
            slots_out[1:1 + HALF, quad] = tile[HALF:]
            slots_out[0, quad] = tile[HALF - 1]
            share(quad).start()
            slots[1:1 + HALF, quad] = tile[:HALF]
            slots[0, quad] = tile[CHIPS - 1]
        return 0

    lax.fori_loop(0, 4, to_slots, 0)

    def gather_own(i, _):
        spots = [33 * i + a for a in range(33)]
        for u in spots:
            found_own[u] = dot(picks[u, :, :CHUNK], slots[u, :8].reshape(CHUNK, TOK)).astype(BF16)
        return 0

    lax.fori_loop(0, (HALF + 1) // 33, gather_own, 0)

    def share_wait(quad, _):
        share(quad).wait()
        return 0

    lax.fori_loop(0, 8, share_wait, 0)

    pick_vals = one_hot(iota((DIM, TOK), 0) + DIM == iota((DIM, TOK), 1))

    def gather_chunks(i, _):
        spots = [33 * i + a for a in range(33)]
        found = [found_own[u].astype(F32) + dot(picks[u, :, CHUNK:], slots[u, 8:].reshape(CHUNK, TOK)) for u in spots]
        for u, rows in zip(spots, found):
            q_wide = rows[:, :DIM]
            inverse = lax.rsqrt(jnp.sum(q_wide * q_wide, axis=1, keepdims=True))
            keys[u] = (q_wide * inverse).astype(BF16)
            narrow = rows.astype(BF16)
            qrows[u] = narrow[:, :DIM]
            vals[u] = dot(pick_vals, narrow, NT).astype(BF16)
        return 0

    lax.fori_loop(0, (HALF + 1) // 33, gather_chunks, 0)
    diagonal = iota((CHUNK, CHUNK), 0) == iota((CHUNK, CHUNK), 1)

    def back_share(n):
        return remote(back_out.at[:, pl.ds(4 * n, 4)], back.at[:, pl.ds(16 + 4 * n, 4)],
                      k_send_sem.at[n], k_recv_sem.at[n], other, chip)

    def softmax(both):
        before, now = both[:CHUNK], jnp.where(diagonal, MASKED, both[CHUNK:])
        top = jnp.maximum(jnp.max(before, axis=0, keepdims=True), jnp.max(now, axis=0, keepdims=True))
        before = jnp.exp2((before - top) * EXP_SCALE)
        now = jnp.exp2((now - top) * EXP_SCALE)
        total = jnp.sum(before, axis=0, keepdims=True) + jnp.sum(now, axis=0, keepdims=True)
        inverse = 1.0 / total
        return jnp.concatenate([(before * inverse).astype(BF16), (now * inverse).astype(BF16)], axis=0)

    def attend(n, _):
        spots = [32 * n + a + 1 for a in range(32)]
        scores = [dot(keys[pl.ds(u - 1, 2)].reshape(2 * CHUNK, DIM), qrows[u], NT) for u in spots]
        probs = [softmax(both) for both in scores]
        outs = [dot(jnp.concatenate([vals[u - 1], vals[u]], axis=1), p).astype(BF16) for u, p in zip(spots, probs)]
        spread = [dot(o, picks[u]) for u, o in zip(spots, outs)]
        for m in range(16):
            tile = jnp.concatenate(spread[2 * m:2 * m + 2], axis=0).T.astype(BF16).reshape(16, 16, TOK)
            back[:, 16 * n + m] = tile[:8]
            back_out[:, 16 * n + m] = tile[8:]

        for part in range(4):
            back_share(part).start()
        return 0

    lax.fori_loop(0, HALF // 32, attend, 0)

    def tokens_own(i, _):
        for a in range(4):
            quad = 4 * i + a
            token_own[quad] = dot(back[quad, :16].reshape(256, TOK), token_hot[quad, :256], TN).astype(BF16)
        return 0

    lax.fori_loop(0, 2, tokens_own, 0)

    def back_wait(n, _):
        back_share(n).wait()
        return 0

    lax.fori_loop(0, 4, back_wait, 0)

    my_batch = place // HEADS
    my_pair = my_batch * HEADS + (chip % 4) * 4 + (chip // 4) % 4

    def to_tokens(i, _):
        quads = [((i // 2 + my_batch) % 2) * 4 + (2 * i + m + chip) % 4 for m in range(2)]
        late = [dot(back[quad, 16:].reshape(256, TOK), token_hot[quad, 256:], TN) for quad in quads]
        for quad, part in zip(quads, late):
            token = core * HALF + quad * 4
            odd = jnp.concatenate([parity[token + a] for a in range(4)], axis=1)
            both = part + token_own[quad].astype(F32)
            rows = jnp.where(odd > 0.5, both[DIM:], both[:DIM]).astype(BF16)
            for a in range(4):
                o_send[quad * 4 + a] = rows[:, a * TOK:(a + 1) * TOK]
        for quad in quads:
            for n in range(4):
                a = (n + chip + chip // 4 + chip // 16) % 4
                target = core * HALF + quad * 4 + a

                @pl.when((target == chip) & mine)
                def _():
                    pltpu.make_async_copy(o_send.at[quad * 4 + a], o_recv.at[my_pair], o_recv_sem.at[my_pair]).start()

                @pl.when((target != chip) | jnp.logical_not(mine))
                def _():
                    remote(o_send.at[quad * 4 + a], o_recv.at[my_pair], o_send_sem, o_recv_sem.at[my_pair], half, target).start()
        return 0

    lax.fori_loop(0, 4, to_tokens, 0)
    my_quad = place // 4

    def arrival(i):
        batch = (i // 4 + my_quad // 4) % 2
        group = (my_quad + 4 - i % 4) % 4
        return batch, group, batch * HEADS + group * 4

    def pass_rows(i):
        rows = pl.ds(arrival(i)[2], 4)
        return remote(o_recv.at[rows], o_far.at[rows], p_send_sem.at[i], p_recv_sem.at[i], other, chip)

    def far_product(i):
        batch, group, first = arrival(i)
        pass_rows(i).wait()
        return dot(o_far[pl.ds(first, 4)].reshape(256, TOK), wo_far[group], TN)

    wo_share.wait()

    def project_out(i, _):
        batch, group, first = arrival(i)
        for n in range(4):
            row = o_recv.at[first + n]
            pltpu.make_async_copy(row, row, o_recv_sem.at[first + n]).wait()
        pass_rows(i).start()
        acc[batch] += dot(o_recv[pl.ds(first, 4)].reshape(256, TOK), wo_buf[group, :, my_columns], TN)

        @pl.when(i > 0)
        def _():
            acc[arrival(i - 1)[0]] += far_product(i - 1)
        return 0

    lax.fori_loop(0, 8, project_out, 0)
    last = arrival(7)[0]
    y_ref[1 - last] = acc[1 - last].astype(BF16)
    y_ref[last] = (acc[last] + far_product(7)).astype(BF16)

    @pl.when(mine)
    def _():
        pltpu.make_async_copy(b_send.at[0:31], b_send.at[0:31], b_send_sem).wait()
        pltpu.make_async_copy(r_send.at[0:31], r_send.at[0:31], r_send_sem).wait()
        pltpu.make_async_copy(o_send.at[0:31], o_send.at[0:31], o_send_sem).wait()

    @pl.when(jnp.logical_not(mine))
    def _():
        pltpu.make_async_copy(b_send, b_send, b_send_sem).wait()
        pltpu.make_async_copy(r_send, r_send, r_send_sem).wait()
        pltpu.make_async_copy(o_send, o_send, o_send_sem).wait()


def solution(mesh):
    def step(hidden, bucket, w_qk, w_v, w_o):
        x = hidden.reshape(2 * TOK, MODEL)
        wq = jnp.transpose(w_qk, (1, 2, 0)).reshape(HEADS * DIM, MODEL)
        wv = jnp.transpose(w_v, (1, 2, 0)).reshape(HEADS * DIM, MODEL)
        wo = w_o.reshape(4, 256, MODEL)
        any_spec = pl.BlockSpec(memory_space=pl.ANY)
        vmem_spec = pl.BlockSpec(memory_space=pltpu.VMEM)
        dma = pltpu.SemaphoreType.DMA
        return pl.pallas_call(
            kernel,
            out_shape=pltpu.VMEM((2, TOK, MODEL // 2), BF16),
            in_specs=[any_spec, vmem_spec, any_spec, any_spec, any_spec],
            out_specs=vmem_spec,
            scratch_shapes=[
                pltpu.VMEM((2 * TOK, MODEL), BF16),
                pltpu.VMEM((4, 2, 256, MODEL), BF16),
                pltpu.VMEM((4, 256, MODEL), BF16),
                pltpu.VMEM((HALF, 1, TOK), jnp.int32),
                pltpu.VMEM((CHIPS, 1, TOK), jnp.int32),
                pltpu.VMEM((HALF, 2 * DIM, TOK), BF16),
                pltpu.VMEM((HALF, 2 * DIM, TOK), BF16),
                pltpu.VMEM((CHIPS, 1, TOK), F32),
                pltpu.VMEM((CHIPS, 1, TOK), F32),
                pltpu.VMEM((CHIPS, 1, TOK), F32),
                pltpu.VMEM((CHIPS, 1, TOK), F32),
                pltpu.VMEM((CHIPS, 256), F32),
                pltpu.VMEM((HALF + 1, 16, 16, TOK), BF16),
                pltpu.VMEM((HALF + 1, 8, 16, TOK), BF16),
                pltpu.VMEM((HALF + 1, CHUNK, 256), BF16),
                pltpu.VMEM((8, 512, 512), BF16),
                pltpu.VMEM((HALF + 1, CHUNK, TOK), BF16),
                pltpu.VMEM((8, TOK, 512), BF16),
                pltpu.VMEM((HALF + 1, CHUNK, DIM), BF16),
                pltpu.VMEM((HALF + 1, DIM, CHUNK), BF16),
                pltpu.VMEM((HALF + 1, CHUNK, DIM), BF16),
                pltpu.VMEM((8, HALF, 16, TOK), BF16),
                pltpu.VMEM((8, HALF // 2, 16, TOK), BF16),
                pltpu.VMEM((HALF, DIM, TOK), BF16),
                pltpu.VMEM((HALF, DIM, TOK), BF16),
                pltpu.VMEM((HALF, DIM, TOK), BF16),
                pltpu.VMEM((4, 256, 1024), BF16),
                pltpu.VMEM((2, TOK, 1024), F32),
                dma((13,)), dma(()), dma(()), dma((2,)), dma(()), dma((HALF,)), dma((8,)), dma((8,)),
                dma((4,)), dma((4,)), dma(()), dma((HALF,)), dma((8,)), dma((8,)), dma((2,)),
            ],
            compiler_params=pltpu.CompilerParams(collective_id=0, has_side_effects=True, vmem_limit_bytes=56 * 1024 * 1024),
            name="bucket_attention",
        )(x, bucket, wq, wv, wo)

    return jax.shard_map(
        step, mesh=mesh,
        in_specs=(P("dp", "sp", None), P("dp", "tp", "sp"), P(None, "tp", None), P(None, "tp", None), P("tp", None, None)),
        out_specs=P("dp", "sp", "tp"), check_vma=False)
```

```python
import functools

import jax
import jax.numpy as jnp
from jax import lax
from jax.experimental import pallas as pl
from jax.experimental.pallas import tpu as pltpu
from jax.sharding import PartitionSpec as P

CHIPS = 64
HALF = 32
TOK = 128
CHUNK = 128
HEADS = 16
DIM = 64
MODEL = 2048
SLOTS = 4
SPAN = 32
MASKED = -8e5
EXP_SCALE = 0.125 * 1.4426950408889634
F32 = jnp.float32
BF16 = jnp.bfloat16
NT = (((1,), (1,)), ((), ()))
TN = (((0,), (0,)), ((), ()))


def iota(shape, axis):
    return lax.broadcasted_iota(jnp.int32, shape, axis)


def one_hot(mask):
    return jnp.where(mask, 1.0, 0.0).astype(BF16)


def dot(a, b, dims=(((1,), (0,)), ((), ()))):
    return lax.dot_general(a, b, dims, preferred_element_type=F32)


def kernel(x_hbm, bucket_ref, wq_hbm, wv_hbm, wo_hbm, y_ref,
           x_buf, w_buf, wo_buf, b_send, b_recv, r_send, r_recv,
           first_rank, code_pair, code_quad, parity, slot_rank,
           slots, slots_out, picks, token_hot, found_own, token_own, keys, vals, qrows, back, back_out, o_send, o_recv, o_far, wo_far, acc,
           load_sem, b_send_sem, b_recv_sem, b_pass_sem, r_send_sem, r_recv_sem, s_send_sem, s_recv_sem,
           k_send_sem, k_recv_sem, o_send_sem, o_recv_sem, p_send_sem, p_recv_sem, w_pass_sem):
    core = lax.axis_index("tp")
    chip = lax.axis_index("sp")
    other = 1 - core
    half = chip // HALF
    place = chip % HALF
    mine = core == half

    def peer(t, s):
        return {"dp": 0, "tp": t, "sp": s}

    def remote(src, dst, send, recv, t, s):
        return pltpu.make_async_remote_copy(
            src_ref=src, dst_ref=dst, send_sem=send, recv_sem=recv,
            device_id=peer(t, s), device_id_type=pl.DeviceIdType.MESH)

    turn = (chip // 8) % 4
    x_load = pltpu.make_async_copy(x_hbm, x_buf, load_sem.at[0])
    x_load.start()

    def w_loads(step):
        group = (step + turn) % 4
        return (pltpu.make_async_copy(wq_hbm.at[pl.ds(group * 256, 256)], w_buf.at[step, 0], load_sem.at[1 + step]),
                pltpu.make_async_copy(wv_hbm.at[pl.ds(group * 256, 256)], w_buf.at[step, 1], load_sem.at[5 + step]))

    for step in range(4):
        for load in w_loads(step):
            load.start()
    wo_loads = [pltpu.make_async_copy(wo_hbm.at[g], wo_buf.at[g], load_sem.at[9 + g]) for g in range(4)]
    for load in wo_loads:
        load.start()

    barrier = pltpu.get_barrier_semaphore()

    def greet(t, s):
        pl.semaphore_signal(barrier, inc=1, device_id=peer(t, s), device_id_type=pl.DeviceIdType.MESH)

    def greet_chip(i, _):
        spot = (place + i) % HALF
        greet(0, core * HALF + spot)
        greet(1, core * HALF + spot)
        greet(half, other * HALF + spot)
        return 0

    lax.fori_loop(1, HALF, greet_chip, 0)
    greet(half, other * HALF + place)
    greet(1 - half, core * HALF + place)

    @pl.when(jnp.logical_not(mine))
    def _():
        greet(half, core * HALF + place)

    for b in range(2):
        for h in range(HEADS):
            b_send[b * HEADS + h] = bucket_ref[b, h:h + 1, :]

    x_load.wait()

    def project(step):
        for load in w_loads(step):
            load.wait()
        group = (step + turn) % 4
        rows = dot(w_buf[step].reshape(512, MODEL), x_buf[...], NT).astype(BF16)
        for hh in range(4):
            for b in range(2):
                pair = b * HEADS + group * 4 + hh
                r_send[pair, 0:DIM] = rows[hh * DIM:(hh + 1) * DIM, b * TOK:(b + 1) * TOK]
                r_send[pair, DIM:2 * DIM] = rows[256 + hh * DIM:256 + (hh + 1) * DIM, b * TOK:(b + 1) * TOK]

    def send_rows(step):
        group = (step + turn) % 4

        def body(i, _):
            spot = (chip // 4 + chip // 16 + 8 - i) % 8
            pair = (spot // 4) * HEADS + group * 4 + spot % 4
            target = core * HALF + (spot // 4) * HEADS + (spot % 4) * 4 + group

            @pl.when((target == chip) & mine)
            def _():
                pltpu.make_async_copy(r_send.at[pair], r_recv.at[place], r_recv_sem.at[place]).start()

            @pl.when((target != chip) | jnp.logical_not(mine))
            def _():
                remote(r_send.at[pair], r_recv.at[place], r_send_sem, r_recv_sem.at[place], half, target).start()
            return 0

        lax.fori_loop(0, 8, body, 0)

    def send_buckets(i, _):
        spot = (i + place) % HALF
        pair = (spot // HEADS) * HEADS + (spot % 4) * 4 + (spot // 4) % 4
        target = core * HALF + spot

        @pl.when((i == 0) & mine)
        def _():
            pltpu.make_async_copy(b_send.at[pair], b_recv.at[chip], b_recv_sem).start()

        @pl.when((i > 0) | jnp.logical_not(mine))
        def _():
            remote(b_send.at[pair], b_recv.at[chip], b_send_sem, b_recv_sem, half, target).start()
        return 0

    project(0)
    acc[...] = jnp.zeros_like(acc)
    @pl.when(mine)
    def _():
        pl.semaphore_wait(barrier, 95)

    @pl.when(jnp.logical_not(mine))
    def _():
        pl.semaphore_wait(barrier, 96)

    lax.fori_loop(0, HALF, send_buckets, 0)
    send_rows(0)

    def project_more(step, _):
        project(step)
        send_rows(step)
        return 0

    lax.fori_loop(1, 4, project_more, 0)

    for load in wo_loads:
        load.wait()
    my_columns = pl.ds(pl.multiple_of(core * 1024, 1024), 1024)
    wo_share = remote(wo_buf.at[:, :, pl.ds(pl.multiple_of(other * 1024, 1024), 1024)], wo_far,
                      w_pass_sem.at[0], w_pass_sem.at[1], other, chip)
    wo_share.start()

    own_rows = b_recv.at[pl.ds(core * HALF, HALF)]
    pltpu.make_async_copy(own_rows, own_rows, b_recv_sem).wait()
    bucket_share = remote(own_rows, own_rows, b_pass_sem.at[0], b_pass_sem.at[1], other, chip)
    bucket_share.start()
    bucket_share.wait()
    lane256 = iota((TOK, 256), 1)
    count_mat = one_hot((lane256 >= TOK) | (iota((TOK, 256), 0) < lane256))
    ids = iota((SPAN, CHIPS, TOK), 1)
    ids_f = ids.astype(F32)

    def rank_first(i, running):
        hot = jnp.where(b_recv[pl.ds(SPAN * i, SPAN)] == ids, 1.0, 0.0)
        counts = dot(hot.astype(BF16).reshape(SPAN * CHIPS, TOK), count_mat)
        for a in range(SPAN):
            block = counts[a * CHIPS:(a + 1) * CHIPS]
            first_rank[SPAN * i + a] = jnp.sum(hot[a] * (block[:, :TOK] + running), axis=0, keepdims=True)
            running = running + block[:, TOK:]
        return running

    totals = lax.fori_loop(0, CHIPS // SPAN, rank_first, jnp.zeros((CHIPS, TOK), F32))
    high = jnp.floor(totals * (1.0 / 64))
    low = totals - 64.0 * high
    below = one_hot(iota((CHIPS, CHIPS), 1) < iota((CHIPS, CHIPS), 0))
    offsets = 64.0 * dot(below, high.astype(BF16)) + dot(below, low.astype(BF16))
    shift = (core * HALF).astype(F32)
    within = iota((SPAN, 1, TOK), 0)
    lane_id = iota((CHIPS, TOK), 1)

    def rank_second(i, chunk_counts):
        hot = jnp.where(b_recv[pl.ds(SPAN * i, SPAN)] == ids, 1.0, 0.0)
        rank = first_rank[pl.ds(SPAN * i, SPAN)] + jnp.sum(hot * offsets[None], axis=1, keepdims=True)
        chunk = jnp.floor(rank * (1.0 / CHUNK)) - shift
        chunk = jnp.where(chunk < 0.0, chunk + float(CHIPS), chunk)
        hot = jnp.where(chunk == ids_f, 1.0, 0.0)
        counts = dot(hot.astype(BF16).reshape(SPAN * CHIPS, TOK), count_mat)
        slot = jnp.sum(hot * counts[:, :TOK].reshape(SPAN, CHIPS, TOK), axis=1, keepdims=True)
        two = jnp.floor(chunk * 0.5)
        code_pair[pl.ds(SPAN * i, SPAN)] = chunk * 8.0 + slot + ((within % 2) * SLOTS).astype(F32)
        code_quad[pl.ds(SPAN * i, SPAN)] = two * 16.0 + slot + ((within % 4) * SLOTS).astype(F32)
        parity[pl.ds(SPAN * i, SPAN)] = chunk - 2.0 * two
        for a in range(SPAN):
            spot = (SPAN * i + a + core * HALF) % CHIPS
            chunk_counts = chunk_counts + jnp.where(lane_id == spot, counts[a * CHIPS:(a + 1) * CHIPS, TOK:], 0.0)
        return chunk_counts

    chunk_counts = lax.fori_loop(0, CHIPS // SPAN, rank_second, jnp.zeros((CHIPS, TOK), F32)).astype(BF16)
    source = iota((TOK, 256), 1) // SLOTS
    sources = iota((TOK, 256), 0)
    base = dot(chunk_counts, one_hot(sources < source))
    filled = dot(chunk_counts, one_hot(sources == source))
    slot_no = (iota((CHIPS, 256), 1) % SLOTS).astype(F32)
    slot_rank[...] = jnp.where(slot_no < filled, base + slot_no, -1.0)

    rank_ids = iota((CHUNK, 256), 0).astype(F32)
    ids_quad = iota((512, 512), 0).astype(F32)

    def make_picks(i, _):
        for a in range(11):
            u = 11 * i + a
            picks[u] = one_hot(slot_rank[pl.ds((u + CHIPS - 1) % CHIPS, 1), :] == rank_ids)
        return 0

    lax.fori_loop(0, (HALF + 1) // 11, make_picks, 0)

    owner_group = chip % 4
    ids512 = iota((512, 256), 0).astype(F32)

    def share(quad):
        return remote(slots_out.at[:, quad], slots.at[:, 8 + quad], s_send_sem.at[quad], s_recv_sem.at[quad], other, chip)

    def to_slots(i, _):
        octet = (owner_group + 4 - i) % 4
        for n in range(8):
            row = r_recv.at[octet * 8 + n]
            pltpu.make_async_copy(row, row, r_recv_sem.at[octet * 8 + n]).wait()
        tiles = []
        for a in range(4):
            spot = octet * 8 + a * 2
            token = core * HALF + spot
            codes = jnp.concatenate([code_pair[token], code_pair[token + 1]], axis=1)
            rows = jnp.concatenate([r_recv[spot], r_recv[spot + 1]], axis=1)
            tiles.append(dot(one_hot(codes == ids512), rows, NT).reshape(CHIPS, 8, TOK))
        for r in range(2):
            quad = 2 * octet + r
            tile = jnp.concatenate(tiles[2 * r:2 * r + 2], axis=1).astype(BF16)
            slots_out[1:1 + HALF, quad] = tile[HALF:]
            slots_out[0, quad] = tile[HALF - 1]
            share(quad).start()
            slots[1:1 + HALF, quad] = tile[:HALF]
            slots[0, quad] = tile[CHIPS - 1]
        return 0

    lax.fori_loop(0, 4, to_slots, 0)

    def gather_own(i, _):
        spots = [33 * i + a for a in range(33)]
        for u in spots:
            found_own[u] = dot(picks[u, :, :CHUNK], slots[u, :8].reshape(CHUNK, TOK)).astype(BF16)
        return 0

    lax.fori_loop(0, (HALF + 1) // 33, gather_own, 0)

    def make_hots(quad, _):
        token = core * HALF + quad * 4
        codes = jnp.concatenate([code_quad[token + a] for a in range(4)], axis=1)
        token_hot[quad] = one_hot(codes == ids_quad)
        return 0

    lax.fori_loop(0, 8, make_hots, 0)

    def share_wait(quad, _):
        share(quad).wait()
        return 0

    lax.fori_loop(0, 8, share_wait, 0)

    pick_vals = one_hot(iota((DIM, TOK), 0) + DIM == iota((DIM, TOK), 1))

    def gather_chunks(i, _):
        spots = [33 * i + a for a in range(33)]
        found = [found_own[u].astype(F32) + dot(picks[u, :, CHUNK:], slots[u, 8:].reshape(CHUNK, TOK)) for u in spots]
        for u, rows in zip(spots, found):
            q_wide = rows[:, :DIM]
            inverse = lax.rsqrt(jnp.sum(q_wide * q_wide, axis=1, keepdims=True))
            keys[u] = (q_wide * inverse).astype(BF16)
            narrow = rows.astype(BF16)
            qrows[u] = narrow[:, :DIM]
            vals[u] = dot(pick_vals, narrow, NT).astype(BF16)
        return 0

    lax.fori_loop(0, (HALF + 1) // 33, gather_chunks, 0)
    diagonal = iota((CHUNK, CHUNK), 0) == iota((CHUNK, CHUNK), 1)

    def back_share(n):
        return remote(back_out.at[:, pl.ds(4 * n, 4)], back.at[:, pl.ds(16 + 4 * n, 4)],
                      k_send_sem.at[n], k_recv_sem.at[n], other, chip)

    def softmax(both):
        before, now = both[:CHUNK], jnp.where(diagonal, MASKED, both[CHUNK:])
        top = jnp.maximum(jnp.max(before, axis=0, keepdims=True), jnp.max(now, axis=0, keepdims=True))
        before = jnp.exp2((before - top) * EXP_SCALE)
        now = jnp.exp2((now - top) * EXP_SCALE)
        total = jnp.sum(before, axis=0, keepdims=True) + jnp.sum(now, axis=0, keepdims=True)
        inverse = 1.0 / total
        return jnp.concatenate([(before * inverse).astype(BF16), (now * inverse).astype(BF16)], axis=0)

    def attend(n, _):
        spots = [32 * n + a + 1 for a in range(32)]
        scores = [dot(keys[pl.ds(u - 1, 2)].reshape(2 * CHUNK, DIM), qrows[u], NT) for u in spots]
        probs = [softmax(both) for both in scores]
        outs = [dot(jnp.concatenate([vals[u - 1], vals[u]], axis=1), p).astype(BF16) for u, p in zip(spots, probs)]
        spread = [dot(o, picks[u]) for u, o in zip(spots, outs)]
        for m in range(16):
            tile = jnp.concatenate(spread[2 * m:2 * m + 2], axis=0).T.astype(BF16).reshape(16, 16, TOK)
            back[:, 16 * n + m] = tile[:8]
            back_out[:, 16 * n + m] = tile[8:]

        for part in range(4):
            back_share(part).start()
        return 0

    lax.fori_loop(0, HALF // 32, attend, 0)

    def tokens_own(i, _):
        for a in range(4):
            quad = 4 * i + a
            token_own[quad] = dot(back[quad, :16].reshape(256, TOK), token_hot[quad, :256], TN).astype(BF16)
        return 0

    lax.fori_loop(0, 2, tokens_own, 0)

    def back_wait(n, _):
        back_share(n).wait()
        return 0

    lax.fori_loop(0, 4, back_wait, 0)

    my_batch = place // HEADS
    my_pair = my_batch * HEADS + (chip % 4) * 4 + (chip // 4) % 4

    def to_tokens(i, _):
        quads = [((i // 2 + my_batch) % 2) * 4 + (2 * i + m + chip) % 4 for m in range(2)]
        late = [dot(back[quad, 16:].reshape(256, TOK), token_hot[quad, 256:], TN) for quad in quads]
        for quad, part in zip(quads, late):
            token = core * HALF + quad * 4
            odd = jnp.concatenate([parity[token + a] for a in range(4)], axis=1)
            both = part + token_own[quad].astype(F32)
            rows = jnp.where(odd > 0.5, both[DIM:], both[:DIM]).astype(BF16)
            for a in range(4):
                o_send[quad * 4 + a] = rows[:, a * TOK:(a + 1) * TOK]
        for quad in quads:
            for n in range(4):
                a = (n + chip + chip // 4 + chip // 16) % 4
                target = core * HALF + quad * 4 + a

                @pl.when((target == chip) & mine)
                def _():
                    pltpu.make_async_copy(o_send.at[quad * 4 + a], o_recv.at[my_pair], o_recv_sem.at[my_pair]).start()

                @pl.when((target != chip) | jnp.logical_not(mine))
                def _():
                    remote(o_send.at[quad * 4 + a], o_recv.at[my_pair], o_send_sem, o_recv_sem.at[my_pair], half, target).start()
        return 0

    lax.fori_loop(0, 4, to_tokens, 0)
    my_quad = place // 4

    def arrival(i):
        batch = (i // 4 + my_quad // 4) % 2
        group = (my_quad + 4 - i % 4) % 4
        return batch, group, batch * HEADS + group * 4

    def pass_rows(i):
        rows = pl.ds(arrival(i)[2], 4)
        return remote(o_recv.at[rows], o_far.at[rows], p_send_sem.at[i], p_recv_sem.at[i], other, chip)

    def far_product(i):
        batch, group, first = arrival(i)
        pass_rows(i).wait()
        return dot(o_far[pl.ds(first, 4)].reshape(256, TOK), wo_far[group], TN)

    wo_share.wait()

    def project_out(i, _):
        batch, group, first = arrival(i)
        for n in range(4):
            row = o_recv.at[first + n]
            pltpu.make_async_copy(row, row, o_recv_sem.at[first + n]).wait()
        pass_rows(i).start()
        acc[batch] += dot(o_recv[pl.ds(first, 4)].reshape(256, TOK), wo_buf[group, :, my_columns], TN)

        @pl.when(i > 0)
        def _():
            acc[arrival(i - 1)[0]] += far_product(i - 1)
        return 0

    lax.fori_loop(0, 8, project_out, 0)
    last = arrival(7)[0]
    y_ref[1 - last] = acc[1 - last].astype(BF16)
    y_ref[last] = (acc[last] + far_product(7)).astype(BF16)

    @pl.when(mine)
    def _():
        pltpu.make_async_copy(b_send.at[0:31], b_send.at[0:31], b_send_sem).wait()
        pltpu.make_async_copy(r_send.at[0:31], r_send.at[0:31], r_send_sem).wait()
        pltpu.make_async_copy(o_send.at[0:31], o_send.at[0:31], o_send_sem).wait()

    @pl.when(jnp.logical_not(mine))
    def _():
        pltpu.make_async_copy(b_send, b_send, b_send_sem).wait()
        pltpu.make_async_copy(r_send, r_send, r_send_sem).wait()
        pltpu.make_async_copy(o_send, o_send, o_send_sem).wait()


def solution(mesh):
    def step(hidden, bucket, w_qk, w_v, w_o):
        x = hidden.reshape(2 * TOK, MODEL)
        wq = jnp.transpose(w_qk, (1, 2, 0)).reshape(HEADS * DIM, MODEL)
        wv = jnp.transpose(w_v, (1, 2, 0)).reshape(HEADS * DIM, MODEL)
        wo = w_o.reshape(4, 256, MODEL)
        any_spec = pl.BlockSpec(memory_space=pl.ANY)
        vmem_spec = pl.BlockSpec(memory_space=pltpu.VMEM)
        dma = pltpu.SemaphoreType.DMA
        return pl.pallas_call(
            kernel,
            out_shape=pltpu.VMEM((2, TOK, MODEL // 2), BF16),
            in_specs=[any_spec, vmem_spec, any_spec, any_spec, any_spec],
            out_specs=vmem_spec,
            scratch_shapes=[
                pltpu.VMEM((2 * TOK, MODEL), BF16),
                pltpu.VMEM((4, 2, 256, MODEL), BF16),
                pltpu.VMEM((4, 256, MODEL), BF16),
                pltpu.VMEM((HALF, 1, TOK), jnp.int32),
                pltpu.VMEM((CHIPS, 1, TOK), jnp.int32),
                pltpu.VMEM((HALF, 2 * DIM, TOK), BF16),
                pltpu.VMEM((HALF, 2 * DIM, TOK), BF16),
                pltpu.VMEM((CHIPS, 1, TOK), F32),
                pltpu.VMEM((CHIPS, 1, TOK), F32),
                pltpu.VMEM((CHIPS, 1, TOK), F32),
                pltpu.VMEM((CHIPS, 1, TOK), F32),
                pltpu.VMEM((CHIPS, 256), F32),
                pltpu.VMEM((HALF + 1, 16, 16, TOK), BF16),
                pltpu.VMEM((HALF + 1, 8, 16, TOK), BF16),
                pltpu.VMEM((HALF + 1, CHUNK, 256), BF16),
                pltpu.VMEM((8, 512, 512), BF16),
                pltpu.VMEM((HALF + 1, CHUNK, TOK), BF16),
                pltpu.VMEM((8, TOK, 512), BF16),
                pltpu.VMEM((HALF + 1, CHUNK, DIM), BF16),
                pltpu.VMEM((HALF + 1, DIM, CHUNK), BF16),
                pltpu.VMEM((HALF + 1, CHUNK, DIM), BF16),
                pltpu.VMEM((8, HALF, 16, TOK), BF16),
                pltpu.VMEM((8, HALF // 2, 16, TOK), BF16),
                pltpu.VMEM((HALF, DIM, TOK), BF16),
                pltpu.VMEM((HALF, DIM, TOK), BF16),
                pltpu.VMEM((HALF, DIM, TOK), BF16),
                pltpu.VMEM((4, 256, 1024), BF16),
                pltpu.VMEM((2, TOK, 1024), F32),
                dma((13,)), dma(()), dma(()), dma((2,)), dma(()), dma((HALF,)), dma((8,)), dma((8,)),
                dma((4,)), dma((4,)), dma(()), dma((HALF,)), dma((8,)), dma((8,)), dma((2,)),
            ],
            compiler_params=pltpu.CompilerParams(collective_id=0, has_side_effects=True, vmem_limit_bytes=56 * 1024 * 1024),
            name="bucket_attention",
        )(x, bucket, wq, wv, wo)

    return jax.shard_map(
        step, mesh=mesh,
        in_specs=(P("dp", "sp", None), P("dp", "tp", "sp"), P(None, "tp", None), P(None, "tp", None), P("tp", None, None)),
        out_specs=P("dp", "sp", "tp"), check_vma=False)
```
